32 devices in a mesh: pod: 1 (over z), data: 4 (over y), col: 4 (over x), row: 2 (over core).
Axes of the slice: x: 4, y: 4, z: 1, core: 2. Of those that a mesh axis runs over, the one named last changes fastest.
The devices are a block of a 4x4x8 slice.
Arguments:
- x_act: bfloat16 [4096, 3072], P(('pod', 'data', 'row'), 'col')
- w_fused: bfloat16 [3072, 16384], P(('pod', 'row'), 'col')
- dy_out: bfloat16 [4096, 16384], P(('pod', 'data', 'row'), 'col')
Outputs:
- output 1: bfloat16 [4096, 3072], P(('pod', 'data', 'row'), 'col')
- output 2: float32 [3072, 16384], P(('pod', 'data', 'row'), 'col')
All inputs are finite; a program needn't handle non-finite values.
Results may differ from the reference program's by a relative error of at most 0.001.
Values are sent between devices in bfloat16 or wider.
A program may use at most 768 MiB of HBM per device.

```python
import jax
import jax.numpy as jnp

HIDDEN = 3072
OUT_COLS = 16384
ROW_COUNT = 4096


def setup_inputs(seed: int = 0, part: int = 0) -> dict:
    part_key = jax.random.fold_in(jax.random.key(seed), part)
    key_act, key_wgt, key_grad = jax.random.split(part_key, 3)
    act_vals = jax.random.normal(key_act, (ROW_COUNT, HIDDEN), jnp.float32) * ROW_COUNT ** -0.5
    wgt_vals = jax.random.normal(key_wgt, (HIDDEN, OUT_COLS), jnp.float32) * OUT_COLS ** -0.5
    grad_vals = jax.random.normal(key_grad, (ROW_COUNT, OUT_COLS), jnp.float32)
    return {"x_act": act_vals.astype(jnp.bfloat16), "w_fused": wgt_vals.astype(jnp.bfloat16), "dy_out": grad_vals.astype(jnp.bfloat16)}


def reference(x_act, w_fused, dy_out):
    dx_full = jnp.dot(dy_out, w_fused.T, preferred_element_type=jnp.float32)
    dw_full = jnp.dot(x_act.T, dy_out, preferred_element_type=jnp.float32)
    return dx_full.astype(jnp.bfloat16), dw_full
```

```python
import functools

import jax
import jax.numpy as jnp
from jax import lax
from jax.experimental import pallas as pl
from jax.experimental.pallas import tpu as pltpu
from jax.sharding import PartitionSpec as P

MESH = pl.DeviceIdType.MESH
NS = 8
NW = 3
NR = 3


def kernel(n, rows, x_ref, w_ref, dy_ref, dx_ref, dw_ref, ws_ref,
           DY, X1, XA, XT, PB, OPP, FULL, WT, RB, RR, DXO,
           lsem, xl, wx, wt, ys, yr, x1s, x1r, x2s, x2r, x3s, x3r, ps, pr, rs, rr, osem, dxs):
    T, O = dy_ref.shape
    F = x_ref.shape[1]
    Q, TH, FH = T // n, T // 2, F // rows
    SW, FT = O // NS, F // NW
    d, c, r = lax.axis_index("data"), lax.axis_index("col"), lax.axis_index("row")

    def mod(v):
        return lax.rem(v + 2 * n, n)

    dp, dm, cp, cm = mod(d + 1), mod(d - 1), mod(c + 1), mod(c - 1)
    sib = 1 - r

    def remote(src, dst, ssem, rsem, **where):
        return pltpu.make_async_remote_copy(src_ref=src, dst_ref=dst, send_sem=ssem, recv_sem=rsem,
                                            device_id=where, device_id_type=MESH)

    barrier = pltpu.get_barrier_semaphore()
    for k in range(1, n):
        pl.semaphore_signal(barrier, inc=1, device_id={"data": mod(d + k)}, device_id_type=MESH)
        pl.semaphore_signal(barrier, inc=1, device_id={"col": mod(c + k)}, device_id_type=MESH)
    pl.semaphore_signal(barrier, inc=1, device_id={"row": sib}, device_id_type=MESH)
    pl.semaphore_wait(barrier, 2 * (n - 1) + 1)

    def cols(s):
        return pl.ds(s * SW, SW)

    def own(s):
        src = DY.at[pl.ds(0, T), cols(s)]
        return (remote(src, DY.at[pl.ds(3 * T, T), cols(s)], ys.at[0, s], yr.at[0, s], data=dp),
                remote(src, DY.at[pl.ds(T, T), cols(s)], ys.at[1, s], yr.at[1, s], data=dm))

    def rel(s):
        return (remote(DY.at[pl.ds(3 * T, TH), cols(s)], DY.at[pl.ds(2 * T, TH), cols(s)], ys.at[2, s], yr.at[2, s], data=dp),
                remote(DY.at[pl.ds(T + TH, TH), cols(s)], DY.at[pl.ds(2 * T + TH, TH), cols(s)], ys.at[3, s], yr.at[3, s], data=dm))

    def load_dy(s):
        return pltpu.make_async_copy(dy_ref.at[:, cols(s)], DY.at[pl.ds(0, T), cols(s)], lsem.at[s])

    w_swap = remote(w_ref, ws_ref, wx.at[0], wx.at[1], row=sib)

    x_keep = pltpu.make_async_copy(x_ref.at[pl.ds(c * Q, Q), :], X1.at[c], xl)
    x1 = [remote(x_ref.at[pl.ds(mod(c + k) * Q, Q), :], X1.at[c], x1s.at[k - 1], x1r.at[k - 1], col=mod(c + k))
          for k in range(1, n)]
    x2 = [remote(X1.at[mod(d + k)], XA.at[c, n - k], x2s.at[k - 1], x2r.at[k - 1], data=mod(d + k))
          for k in range(1, n)]
    x3 = [remote(XA.at[c, pl.ds(1, n - 1)], XA.at[c, pl.ds(1, n - 1)], x3s.at[0], x3r.at[0], col=cp),
          remote(XA.at[c, pl.ds(1, n - 1)], XA.at[c, pl.ds(1, n - 1)], x3s.at[1], x3r.at[1], col=cm),
          remote(X1.at[d], XA.at[c, 0], x3s.at[2], x3r.at[2], col=cp),
          remote(X1.at[d], XA.at[c, 0], x3s.at[3], x3r.at[3], col=cm)]
    x4 = [remote(XA.at[cm, pl.ds(0, 2)], XA.at[cm, pl.ds(0, 2)], x3s.at[4], x3r.at[4], col=cp),
          remote(XA.at[cp, pl.ds(2, 2)], XA.at[cp, pl.ds(2, 2)], x3s.at[5], x3r.at[5], col=cm)]

    lo, hi = pl.ds(0, TH), pl.ds(TH, TH)
    opp = [remote(PB.at[0, lo], OPP.at[0], ps.at[0], pr.at[0], col=cm),
           remote(PB.at[0, hi], OPP.at[1], ps.at[1], pr.at[1], col=cp)]
    now = [remote(PB.at[1, hi], FULL.at[0, hi], ps.at[2], pr.at[2], col=cm),
           remote(PB.at[2, lo], FULL.at[1, lo], ps.at[3], pr.at[3], col=cp)]
    late = [remote(PB.at[1, lo], FULL.at[0, lo], ps.at[4], pr.at[4], col=cm),
            remote(PB.at[2, hi], FULL.at[1, hi], ps.at[5], pr.at[5], col=cp)]

    def part(s):
        return remote(RB.at[s % NR, pl.ds(sib * FH, FH)], RR.at[s], rs.at[s], rr.at[s], row=sib)

    def put(s):
        return pltpu.make_async_copy(RB.at[s % NR, pl.ds(r * FH, FH)], dw_ref.at[:, cols(s)], osem.at[s])

    def start(copies):
        for copy in copies:
            copy.start()

    def arrive(copies):
        for copy in copies:
            copy.wait_recv()

    target = [mod(c + 2), cm, cp, c]
    per = n // rows

    def tile_wait(i):
        pltpu.make_async_copy(w_ref.at[pl.ds(0, FT), :], WT.at[i], wt.at[i]).wait()

    def tile_start(k, i):
        b = target[k]
        row0 = pl.multiple_of(lax.rem(b, per) * F + i * FT, FT)

        @pl.when(b // per == r)
        def _():
            pltpu.make_async_copy(w_ref.at[pl.ds(row0, FT), :], WT.at[i], wt.at[i]).start()

        @pl.when(b // per != r)
        def _():
            pltpu.make_async_copy(ws_ref.at[pl.ds(row0, FT), :], WT.at[i], wt.at[i]).start()

    def dx_block(k):
        def one(i, carry):
            tile_wait(i)
            PB[k, :, pl.ds(pl.multiple_of(i * FT, FT), FT)] = lax.dot_general(
                DY[pl.ds(0, T), :], WT[i], (((1,), (1,)), ((), ())), preferred_element_type=jnp.float32)
            if k + 1 < n:
                tile_start(k + 1, i)
            return carry

        lax.fori_loop(0, NW, one, 0)

    def dw_slice(s):
        half = SW // 2

        def one(i, carry):
            RB[s % NR, :, pl.ds(pl.multiple_of(i * half, half), half)] = lax.dot_general(
                XT[...], DY[:, pl.ds(pl.multiple_of(s * SW + i * half, half), half)],
                (((1,), (0,)), ((), ())), preferred_element_type=jnp.float32)
            return carry

        lax.fori_loop(0, 2, one, 0)

    def dw_finish(s):
        part(s).wait_recv()
        keep = pl.ds(pl.multiple_of(r * FH, FH), FH)
        RB[s % NR, keep] = RB[s % NR, keep] + RR[s]
        put(s).start()

    for s in range(NS):
        load_dy(s).start()
    x_keep.start()
    start(x1)
    w_swap.start()
    for s in range(2):
        load_dy(s).wait()
        start(own(s))
    x_keep.wait()
    arrive(x1)
    start(x2)
    for s in range(2, NS):
        load_dy(s).wait()
    start(own(2))
    XA[c, 0] = X1[d]
    arrive(own(0))
    start(rel(0))
    start(own(3))
    arrive(own(1))
    start(rel(1))
    start(own(4))
    arrive(x2)
    start(x3)
    w_swap.wait_recv()
    for i in range(NW):
        tile_start(0, i)
    dx_block(0)
    dx_block(1)
    arrive(own(2))
    start(rel(2))
    start(own(5))
    dx_block(2)
    arrive(x3)
    start(x4)
    start(opp)
    start(now)
    dx_block(3)
    arrive(own(3))
    start(rel(3))
    start(own(6))
    arrive(x4)
    for k in range(n):
        for j in range(n):
            XT[:, pl.ds((k * n + j) * Q, Q)] = XA[j, k].T

    for s in range(NS):
        if 2 <= s < NS - 2:
            arrive(own(s + 2))
            start(rel(s + 2))
            if s + 5 < NS:
                start(own(s + 5))
        if s == 3:
            arrive(opp)
            PB[1, lo] = PB[1, lo] + OPP[0]
            PB[2, hi] = PB[2, hi] + OPP[1]
        if s == 6:
            arrive(now)
            arrive(late)
            DXO[...] = (PB[3] + FULL[0] + FULL[1]).astype(DXO.dtype)
            pltpu.make_async_copy(DXO, dx_ref, dxs).start()
        arrive(rel(s))
        if s >= NR:
            part(s - NR).wait_send()
            put(s - NR).wait()
        dw_slice(s)
        if s == 3:
            start(late)
        if s > 0:
            dw_finish(s - 1)
        part(s).start()
    dw_finish(NS - 1)

    for s in range(NS):
        for copy in own(s) + rel(s):
            copy.wait_send()
    for copy in [w_swap] + x1 + x2 + x3 + x4 + opp + now + late:
        copy.wait_send()
    for s in range(NS - NR, NS):
        part(s).wait_send()
        put(s).wait()
    pltpu.make_async_copy(DXO, dx_ref, dxs).wait()


def solution(mesh):
    n, rows = mesh.shape["col"], mesh.shape["row"]
    assert n == 4 and mesh.shape["data"] == n and rows == 2
    act_spec = P(("pod", "data", "row"), "col")
    wgt_spec = P(("pod", "row"), "col")

    def local_step(x, w, dy):
        T, O = dy.shape
        F = x.shape[1]
        Q, TH, FH, SW = T // n, T // 2, F // rows, O // NS
        bf16, f32 = jnp.bfloat16, jnp.float32
        dma = pltpu.SemaphoreType.DMA
        any_spec = pl.BlockSpec(memory_space=pl.ANY)
        dx, dw, _ = pl.pallas_call(
            functools.partial(kernel, n, rows),
            out_shape=[jax.ShapeDtypeStruct((T, F), bf16), jax.ShapeDtypeStruct((FH, O), f32),
                       jax.ShapeDtypeStruct(w.shape, bf16)],
            in_specs=[any_spec] * 3,
            out_specs=[any_spec] * 3,
            scratch_shapes=[
                pltpu.VMEM((n * T, O), bf16),
                pltpu.VMEM((n, Q, F), bf16),
                pltpu.VMEM((n, n, Q, F), bf16),
                pltpu.VMEM((F, n * T), bf16),
                pltpu.VMEM((n, T, F), f32),
                pltpu.VMEM((2, TH, F), f32),
                pltpu.VMEM((2, T, F), f32),
                pltpu.VMEM((NW, F // NW, O), bf16),
                pltpu.VMEM((NR, F, SW), f32),
                pltpu.VMEM((NS, FH, SW), f32),
                pltpu.VMEM((T, F), bf16),
                dma((NS,)), dma, dma((2,)), dma((NW,)), dma((4, NS)), dma((4, NS)),
                dma((n - 1,)), dma((n - 1,)), dma((n - 1,)), dma((n - 1,)), dma((6,)), dma((6,)),
                dma((6,)), dma((6,)), dma((NS,)), dma((NS,)), dma((NS,)), dma,
            ],
            compiler_params=pltpu.CompilerParams(
                collective_id=0, has_side_effects=True, vmem_limit_bytes=67043328),
            cost_estimate=pl.CostEstimate(flops=8 * T * F * O * n // 2, bytes_accessed=4 * T * O, transcendentals=0),
        )(x, w, dy)
        return dx, dw

    return jax.shard_map(local_step, mesh=mesh, in_specs=(act_spec, wgt_spec, act_spec), out_specs=(act_spec, act_spec),
                         check_vma=False)
```

```python
import functools

import jax
import jax.numpy as jnp
from jax import lax
from jax.experimental import pallas as pl
from jax.experimental.pallas import tpu as pltpu
from jax.sharding import PartitionSpec as P

MESH = pl.DeviceIdType.MESH
NS = 4
NW = 3


def kernel(n, rows, x_ref, w_ref, dy_ref, dx_ref, dw_ref, ws_ref,
           DY, X0, X1, XA, XTP, XTD, RP, PB, OPP, FULL, WT,
           lsem, x0s, wx, wt, os, gs, gr, fs, fr, x1s, x1r, x2s, x2r, x3s, x3r, ps, pr, rs, rr):
    T, O = dy_ref.shape
    F = x_ref.shape[1]
    CT, TH, FH = rows * T, T // 2, F // rows
    QT, QH = CT // n, CT // n // 2
    SW, FT = O // (2 * NS), F // NW
    d, c, r = lax.axis_index("data"), lax.axis_index("col"), lax.axis_index("row")

    def mod(v):
        return lax.rem(v + 2 * n, n)

    cp, cm, sib = mod(c + 1), mod(c - 1), 1 - r
    pair = [d + 1 - 2 * lax.rem(d, 2), n - 1 - d]
    far = mod(d + 2)

    def remote(src, dst, ssem, rsem, **where):
        return pltpu.make_async_remote_copy(src_ref=src, dst_ref=dst, send_sem=ssem, recv_sem=rsem,
                                            device_id=where, device_id_type=MESH)

    def start(copies):
        for copy in copies:
            copy.start()

    def arrive(copies):
        for copy in copies:
            copy.wait_recv()

    barrier = pltpu.get_barrier_semaphore()
    peers = [{"row": sib}] + [{"data": p} for p in pair] + [{"col": mod(c + k)} for k in range(1, n)]
    for peer in peers:
        pl.semaphore_signal(barrier, inc=1, device_id=peer, device_id_type=MESH)
    pl.semaphore_wait(barrier, len(peers))

    mine = pl.ds(pl.multiple_of(r * T, T), T)
    other = pl.ds(pl.multiple_of(CT + r * T, T), T)

    def cols(h, s):
        return pl.ds(h * (O // 2) + s * SW, SW)

    def load_dy(h, s):
        return pltpu.make_async_copy(dy_ref.at[:, cols(h, s)], DY.at[mine, cols(h, s)], lsem.at[h, s])

    def gather(h, s):
        return remote(DY.at[mine, cols(h, s)], DY.at[other, cols(h, s)], gs.at[h, s], gr.at[h, s], data=pair[h])

    def forward(h, s):
        return remote(DY.at[other, cols(h, s)], DY.at[other, cols(h, s)], fs.at[h, s], fr.at[h, s], row=sib)

    own_dy = remote(DY.at[mine, :], DY.at[mine, :], os.at[0], os.at[1], row=sib)
    w_swap = remote(w_ref, ws_ref, wx.at[0], wx.at[1], row=sib)

    def feats(row):
        return pl.ds(pl.multiple_of(row * FH, FH), FH)

    x_keep = pltpu.make_async_copy(x_ref.at[:, feats(r)], X0.at[mine, :], x0s.at[0])
    x_swap = remote(x_ref.at[:, feats(sib)], X0.at[mine, :], x0s.at[1], x0s.at[2], row=sib)

    def quarter(j):
        return pl.ds(pl.multiple_of(j * QT, QT), QT)

    x1 = [remote(X0.at[quarter(mod(c + k)), :], X1.at[c], x1s.at[k - 1], x1r.at[k - 1], col=mod(c + k))
          for k in range(1, n)]
    x2a = [remote(X1.at[far], XA.at[2 + h, c], x2s.at[h], x2r.at[h], data=pair[h]) for h in range(2)]
    x2b = [remote(X1.at[pair[h]], XA.at[5 + h, c], x2s.at[2 + h], x2r.at[2 + h], data=pair[h]) for h in range(2)]

    slots = iter(range(64))

    def spread(src, dst):
        k, m = next(slots), next(slots)
        return [remote(src, dst, x3s.at[k], x3r.at[k], col=cp), remote(src, dst, x3s.at[m], x3r.at[m], col=cm)]

    def hand_on(right, left):
        k, m = next(slots), next(slots)
        return [remote(right, right, x3s.at[k], x3r.at[k], col=cp), remote(left, left, x3s.at[m], x3r.at[m], col=cm)]

    x3i = spread(X1.at[pair[1]], XA.at[0, c]) + spread(X1.at[pair[0]], XA.at[1, c])
    x4i = hand_on(XA.at[0, cm], XA.at[1, cp])
    x3ii = spread(XA.at[pl.ds(2, 2), c], XA.at[pl.ds(2, 2), c])
    x4ii = hand_on(XA.at[2, cm], XA.at[3, cp])
    x3iii = spread(X1.at[d], XA.at[4, c]) + spread(XA.at[pl.ds(5, 2), c], XA.at[pl.ds(5, 2), c])
    x4iii = (hand_on(XA.at[5, cm], XA.at[6, cp])
             + hand_on(XA.at[4, cm, pl.ds(0, QH)], XA.at[4, cp, pl.ds(QH, QH)]))

    lo, hi = pl.ds(0, TH), pl.ds(TH, TH)
    opp = [remote(PB.at[0, lo], OPP.at[0], ps.at[0], pr.at[0], col=cm),
           remote(PB.at[0, hi], OPP.at[1], ps.at[1], pr.at[1], col=cp)]
    now = [remote(PB.at[1, hi], FULL.at[0, hi], ps.at[2], pr.at[2], col=cm),
           remote(PB.at[2, lo], FULL.at[1, lo], ps.at[3], pr.at[3], col=cp)]
    late = [remote(PB.at[1, lo], FULL.at[0, lo], ps.at[4], pr.at[4], col=cm),
            remote(PB.at[2, hi], FULL.at[1, hi], ps.at[5], pr.at[5], col=cp)]

    def total(h, s):
        return remote(RP.at[h * NS + s], dw_ref.at[:, cols(h, s)], rs.at[h, s], rr.at[h, s], data=pair[1 - h])

    target = [mod(c + 2), cm, cp, c]
    per = n // rows

    def tile_wait(i):
        pltpu.make_async_copy(w_ref.at[pl.ds(0, FT), :], WT.at[i], wt.at[i]).wait()

    def tile_start(k, i):
        b = target[k]
        row0 = pl.multiple_of(lax.rem(b, per) * F + i * FT, FT)

        @pl.when(b // per == r)
        def _():
            pltpu.make_async_copy(w_ref.at[pl.ds(row0, FT), :], WT.at[i], wt.at[i]).start()

        @pl.when(b // per != r)
        def _():
            pltpu.make_async_copy(ws_ref.at[pl.ds(row0, FT), :], WT.at[i], wt.at[i]).start()

    def dx_block(k):
        def one(i, carry):
            tile_wait(i)
            PB[k, :, pl.ds(pl.multiple_of(i * FT, FT), FT)] = lax.dot_general(
                DY[mine, :], WT[i], (((1,), (1,)), ((), ())), preferred_element_type=jnp.float32)
            if k + 1 < n:
                tile_start(k + 1, i)
            return carry

        lax.fori_loop(0, NW, one, 0)

    half = SW // 2

    def product(xt, h, s, i):
        return lax.dot_general(xt, DY[:, pl.ds(pl.multiple_of(h * (O // 2) + s * SW + i * half, half), half)],
                               (((1,), (0,)), ((), ())), preferred_element_type=jnp.float32)

    def dw_part(xt, h, s, slot):
        def one(i, carry):
            RP[slot, :, pl.ds(pl.multiple_of(i * half, half), half)] = product(xt[h], h, s, i)
            return carry

        lax.fori_loop(0, 2, one, 0)

    def dw_add(h, s):
        def one(i, carry):
            at = pl.ds(pl.multiple_of(h * (O // 2) + s * SW + i * half, half), half)
            dw_ref[:, at] = dw_ref[:, at] + product(XTD[h], h, s, i)
            return carry

        lax.fori_loop(0, 2, one, 0)

    def turn(block, places):
        for j in range(n):
            value = XA[block, j].T
            for ref, h, side in places:
                ref[h, :, pl.ds(side * CT + j * QT, QT)] = value

    both = range(2)
    x_keep.start()
    x_swap.start()
    for s in range(NS):
        for h in both:
            load_dy(h, s).start()
    w_swap.start()
    for h in both:
        load_dy(h, 0).wait()
        gather(h, 0).start()
    x_keep.wait()
    x_swap.wait_recv()
    start(x1)
    X1[c] = X0[quarter(c), :]
    for s in range(1, NS):
        for h in both:
            load_dy(h, s).wait()
    own_dy.start()
    arrive(x1)
    start(x3i)
    start(x2a)
    for h in both:
        gather(h, 1).start()
    start(x2b)
    for s in range(2, NS):
        for h in both:
            gather(h, s).start()
    XA[0, c] = X1[pair[1]]
    XA[1, c] = X1[pair[0]]
    XA[4, c] = X1[d]
    for h in both:
        gather(h, 0).wait_recv()
        forward(h, 0).start()
    arrive(x2a)
    start(x3ii)
    arrive(x3i)
    start(x4i)
    w_swap.wait_recv()
    for i in range(NW):
        tile_start(0, i)
    dx_block(0)
    for h in both:
        gather(h, 1).wait_recv()
        forward(h, 1).start()
    arrive(x3ii)
    start(x4ii)
    dx_block(1)
    arrive(x2b)
    start(x3iii)
    dx_block(2)
    arrive(x4i)
    turn(0, [(XTP, 0, 0)])
    turn(1, [(XTP, 1, 0)])
    arrive(x4ii)
    turn(2, [(XTP, 0, 1)])
    turn(3, [(XTP, 1, 1)])
    own_dy.wait_recv()
    for s in range(NS):
        if s + 2 < NS:
            for h in both:
                gather(h, s + 2).wait_recv()
                forward(h, s + 2).start()
        for h in both:
            forward(h, s).wait_recv()
            dw_part(XTP, h, s, h * NS + s)
        if s == 1:
            arrive(x3iii)
            start(x4iii)
            start(opp)
            start(now)
        for h in both:
            total(h, s).start()
    dx_block(3)
    arrive(x4iii)
    turn(4, [(XTD, 0, 0), (XTD, 1, 0)])
    turn(5, [(XTD, 0, 1)])
    turn(6, [(XTD, 1, 1)])
    for s in range(NS):
        if s == 1:
            arrive(opp)
            PB[1, lo] = PB[1, lo] + OPP[0]
            PB[2, hi] = PB[2, hi] + OPP[1]
        if s == NS - 1:
            for h in both:
                total(h, 0).wait_send()
                dw_part(XTD, h, s, h * NS)
            arrive(now)
            arrive(late)
            dx_ref[...] = (PB[3] + FULL[0] + FULL[1]).astype(dx_ref.dtype)
        for h in both:
            total(h, s).wait_recv()
            if s == NS - 1:
                dw_ref[:, cols(h, s)] = dw_ref[:, cols(h, s)] + RP[h * NS]
            else:
                dw_add(h, s)
        if s == 1:
            start(late)

    for s in range(NS):
        for h in both:
            gather(h, s).wait_send()
            forward(h, s).wait_send()
            if s > 0:
                total(h, s).wait_send()
    for copy in [w_swap, own_dy, x_swap] + x1 + x2a + x2b + x3i + x4i + x3ii + x4ii + x3iii + x4iii + opp + now + late:
        copy.wait_send()


def solution(mesh):
    n, rows = mesh.shape["col"], mesh.shape["row"]
    assert n == 4 and mesh.shape["data"] == n and rows == 2
    act_spec = P(("pod", "data", "row"), "col")
    wgt_spec = P(("pod", "row"), "col")

    def local_step(x, w, dy):
        T, O = dy.shape
        F = x.shape[1]
        CT, FH = rows * T, F // rows
        QT, SW = CT // n, O // (2 * NS)
        bf16, f32 = jnp.bfloat16, jnp.float32
        dma = pltpu.SemaphoreType.DMA
        any_spec = pl.BlockSpec(memory_space=pl.ANY)
        vmem_spec = pl.BlockSpec(memory_space=pltpu.VMEM)
        dx, dw, _ = pl.pallas_call(
            functools.partial(kernel, n, rows),
            out_shape=[pltpu.VMEM((T, F), bf16), pltpu.VMEM((FH, O), f32), jax.ShapeDtypeStruct(w.shape, bf16)],
            in_specs=[any_spec] * 3,
            out_specs=[vmem_spec, vmem_spec, any_spec],
            scratch_shapes=[
                pltpu.VMEM((2 * CT, O), bf16),
                pltpu.VMEM((CT, FH), bf16),
                pltpu.VMEM((n, QT, FH), bf16),
                pltpu.VMEM((7, n, QT, FH), bf16),
                pltpu.VMEM((2, FH, 2 * CT), bf16),
                pltpu.VMEM((2, FH, 2 * CT), bf16),
                pltpu.VMEM((2 * NS, FH, SW), f32),
                pltpu.VMEM((n, T, F), f32),
                pltpu.VMEM((2, T // 2, F), f32),
                pltpu.VMEM((2, T, F), f32),
                pltpu.VMEM((NW, F // NW, O), bf16),
                dma((2, NS)), dma((3,)), dma((2,)), dma((NW,)), dma((2,)),
                dma((2, NS)), dma((2, NS)), dma((2, NS)), dma((2, NS)),
                dma((n - 1,)), dma((n - 1,)), dma((4,)), dma((4,)), dma((18,)), dma((18,)),
                dma((6,)), dma((6,)), dma((2, NS)), dma((2, NS)),
            ],
            compiler_params=pltpu.CompilerParams(
                collective_id=0, has_side_effects=True, vmem_limit_bytes=58 * 1000 * 1000),
            cost_estimate=pl.CostEstimate(flops=16 * T * F * O * n // 4, bytes_accessed=4 * T * O, transcendentals=0),
        )(x, w, dy)
        return dx, dw

    return jax.shard_map(local_step, mesh=mesh, in_specs=(act_spec, wgt_spec, act_spec), out_specs=(act_spec, act_spec),
                         check_vma=False)
```

```python
import functools

import jax
import jax.numpy as jnp
from jax import lax
from jax.experimental import pallas as pl
from jax.experimental.pallas import tpu as pltpu
from jax.sharding import PartitionSpec as P

MESH = pl.DeviceIdType.MESH
NS = 4
NW = 3


def kernel(n, rows, x_ref, w_ref, dy_ref, dx_ref, dw_ref, end_ref, ws_ref,
           DY, X0, X1, XA, XTP, XTD, RP, PB, OPP, FULL, WT,
           lsem, x0s, wx, wt, os, gs, gr, fs, fr, x1s, x1r, x2s, x2r, x3s, x3r, ps, pr, rs, rr):
    T, O = dy_ref.shape
    F = x_ref.shape[1]
    CT, TH, FH = rows * T, T // 2, F // rows
    QT, QH = CT // n, CT // n // 2
    SW, FT = O // (2 * NS), F // NW
    d, c, r = lax.axis_index("data"), lax.axis_index("col"), lax.axis_index("row")

    def mod(v):
        return lax.rem(v + 2 * n, n)

    cp, cm, sib = mod(c + 1), mod(c - 1), 1 - r
    pair = [d + 1 - 2 * lax.rem(d, 2), n - 1 - d]
    far = mod(d + 2)

    def remote(src, dst, ssem, rsem, **where):
        return pltpu.make_async_remote_copy(src_ref=src, dst_ref=dst, send_sem=ssem, recv_sem=rsem,
                                            device_id=where, device_id_type=MESH)

    def start(copies):
        for copy in copies:
            copy.start()

    def arrive(copies):
        for copy in copies:
            copy.wait_recv()

    mine = pl.ds(pl.multiple_of(r * T, T), T)
    other = pl.ds(pl.multiple_of(CT + r * T, T), T)

    def cols(h, s):
        return pl.ds(h * (O // 2) + s * SW, SW)

    def load_dy(h, s):
        return pltpu.make_async_copy(dy_ref.at[:, cols(h, s)], DY.at[mine, cols(h, s)], lsem.at[h, s])

    def gather(h, s):
        return remote(DY.at[mine, cols(h, s)], DY.at[other, cols(h, s)], gs.at[h, s], gr.at[h, s], data=pair[h])

    def forward(h, s):
        return remote(DY.at[other, cols(h, s)], DY.at[other, cols(h, s)], fs.at[h, s], fr.at[h, s], row=sib)

    own_dy = remote(DY.at[mine, :], DY.at[mine, :], os.at[0], os.at[1], row=sib)
    w_swap = remote(w_ref, ws_ref, wx.at[0], wx.at[1], row=sib)

    def feats(row):
        return pl.ds(pl.multiple_of(row * FH, FH), FH)

    x_keep = pltpu.make_async_copy(x_ref.at[:, feats(r)], X0.at[mine, :], x0s.at[0])
    x_swap = remote(x_ref.at[:, feats(sib)], X0.at[mine, :], x0s.at[1], x0s.at[2], row=sib)

    def quarter(j):
        return pl.ds(pl.multiple_of(j * QT, QT), QT)

    x1 = [remote(X0.at[quarter(mod(c + k)), :], X1.at[c], x1s.at[k - 1], x1r.at[k - 1], col=mod(c + k))
          for k in range(1, n)]
    x2a = [remote(X1.at[far], XA.at[2 + h, c], x2s.at[h], x2r.at[h], data=pair[h]) for h in range(2)]
    x2b = [remote(X1.at[pair[h]], XA.at[5 + h, c], x2s.at[2 + h], x2r.at[2 + h], data=pair[h]) for h in range(2)]

    slots = iter(range(64))

    def spread(src, dst):
        k, m = next(slots), next(slots)
        return [remote(src, dst, x3s.at[k], x3r.at[k], col=cp), remote(src, dst, x3s.at[m], x3r.at[m], col=cm)]

    def hand_on(right, left):
        k, m = next(slots), next(slots)
        return [remote(right, right, x3s.at[k], x3r.at[k], col=cp), remote(left, left, x3s.at[m], x3r.at[m], col=cm)]

    x3i = spread(X1.at[pair[1]], XA.at[0, c]) + spread(X1.at[pair[0]], XA.at[1, c])
    x4i = hand_on(XA.at[0, cm], XA.at[1, cp])
    x3ii = spread(XA.at[pl.ds(2, 2), c], XA.at[pl.ds(2, 2), c])
    x4ii = hand_on(XA.at[2, cm], XA.at[3, cp])
    x3iii = spread(X1.at[d], XA.at[4, c]) + spread(XA.at[pl.ds(5, 2), c], XA.at[pl.ds(5, 2), c])
    x4iii = (hand_on(XA.at[5, cm], XA.at[6, cp])
             + hand_on(XA.at[4, cm, pl.ds(0, QH)], XA.at[4, cp, pl.ds(QH, QH)]))

    lo, hi = pl.ds(0, TH), pl.ds(TH, TH)
    opp = [remote(PB.at[0, lo], OPP.at[0], ps.at[0], pr.at[0], col=cm),
           remote(PB.at[0, hi], OPP.at[1], ps.at[1], pr.at[1], col=cp)]
    now = [remote(PB.at[1, hi], FULL.at[0, hi], ps.at[2], pr.at[2], col=cm),
           remote(PB.at[2, lo], FULL.at[1, lo], ps.at[3], pr.at[3], col=cp)]
    late = [remote(PB.at[1, lo], FULL.at[0, lo], ps.at[4], pr.at[4], col=cm),
            remote(PB.at[2, hi], FULL.at[1, hi], ps.at[5], pr.at[5], col=cp)]

    def total(h, s):
        return remote(RP.at[h * NS + s], dw_ref.at[:, cols(h, s)], rs.at[h, s], rr.at[h, s], data=pair[1 - h])

    target = [mod(c + 2), cm, cp, c]
    per = n // rows

    def tile_wait(i):
        pltpu.make_async_copy(w_ref.at[pl.ds(0, FT), :], WT.at[i], wt.at[i]).wait()

    def tile_start(k, i):
        b = target[k]
        row0 = pl.multiple_of(lax.rem(b, per) * F + i * FT, FT)

        @pl.when(b // per == r)
        def _():
            pltpu.make_async_copy(w_ref.at[pl.ds(row0, FT), :], WT.at[i], wt.at[i]).start()

        @pl.when(b // per != r)
        def _():
            pltpu.make_async_copy(ws_ref.at[pl.ds(row0, FT), :], WT.at[i], wt.at[i]).start()

    def dx_block(k):
        def one(i, carry):
            tile_wait(i)
            PB[k, :, pl.ds(pl.multiple_of(i * FT, FT), FT)] = lax.dot_general(
                DY[mine, :], WT[i], (((1,), (1,)), ((), ())), preferred_element_type=jnp.float32)
            if k + 1 < n:
                tile_start(k + 1, i)
            return carry

        lax.fori_loop(0, NW, one, 0)

    half = SW // 2

    def product(xt, h, s, i):
        return lax.dot_general(xt, DY[:, pl.ds(pl.multiple_of(h * (O // 2) + s * SW + i * half, half), half)],
                               (((1,), (0,)), ((), ())), preferred_element_type=jnp.float32)

    def dw_part(xt, h, s, out, slot):
        def one(i, carry):
            out[slot, :, pl.ds(pl.multiple_of(i * half, half), half)] = product(xt[h], h, s, i)
            return carry

        lax.fori_loop(0, 2, one, 0)

    def dw_add(h, s):
        def one(i, carry):
            at = pl.ds(pl.multiple_of(h * (O // 2) + s * SW + i * half, half), half)
            dw_ref[:, at] = dw_ref[:, at] + product(XTD[h], h, s, i)
            return carry

        lax.fori_loop(0, 2, one, 0)

    def turn(block, places):
        for j in range(n):
            value = XA[block, j].T
            for ref, h, side in places:
                ref[h, :, pl.ds(side * CT + j * QT, QT)] = value

    both = range(2)
    for s in range(NS):
        for h in both:
            load_dy(h, s).start()
    x_keep.start()
    barrier = pltpu.get_barrier_semaphore()
    peers = [{"row": sib}] + [{"data": p} for p in pair] + [{"col": mod(c + k)} for k in range(1, n)]
    for peer in peers:
        pl.semaphore_signal(barrier, inc=1, device_id=peer, device_id_type=MESH)
    pl.semaphore_wait(barrier, len(peers))

    x_swap.start()
    for s in range(2):
        for h in both:
            load_dy(h, s).wait()
            gather(h, s).start()
    w_swap.start()
    x_keep.wait()
    x_swap.wait_recv()
    start(x1)
    X1[c] = X0[quarter(c), :]
    for s in range(2, NS):
        for h in both:
            load_dy(h, s).wait()
    own_dy.start()
    arrive(x1)
    start(x3i)
    start(x2a)
    start(x2b)
    for s in range(2, NS):
        for h in both:
            gather(h, s).start()
    XA[0, c] = X1[pair[1]]
    XA[1, c] = X1[pair[0]]
    XA[4, c] = X1[d]
    for h in both:
        gather(h, 0).wait_recv()
        forward(h, 0).start()
    arrive(x2a)
    start(x3ii)
    arrive(x3i)
    start(x4i)
    w_swap.wait_recv()
    for i in range(NW):
        tile_start(0, i)
    dx_block(0)
    for h in both:
        gather(h, 1).wait_recv()
        forward(h, 1).start()
    arrive(x3ii)
    start(x4ii)
    dx_block(1)
    arrive(x2b)
    start(x3iii)
    dx_block(2)
    arrive(x4i)
    turn(0, [(XTP, 0, 0)])
    turn(1, [(XTP, 1, 0)])
    arrive(x4ii)
    turn(2, [(XTP, 0, 1)])
    turn(3, [(XTP, 1, 1)])
    own_dy.wait_recv()
    for s in range(NS):
        if s + 2 < NS:
            for h in both:
                gather(h, s + 2).wait_recv()
                forward(h, s + 2).start()
        for h in both:
            forward(h, s).wait_recv()
            dw_part(XTP, h, s, RP, h * NS + s)
        if s == 1:
            arrive(x3iii)
            start(x4iii)
            start(opp)
            start(now)
        for h in both:
            total(h, s).start()
    dx_block(3)
    arrive(x4iii)
    turn(4, [(XTD, 0, 0), (XTD, 1, 0)])
    turn(5, [(XTD, 0, 1)])
    turn(6, [(XTD, 1, 1)])
    for s in range(NS):
        if s == 1:
            arrive(opp)
            PB[1, lo] = PB[1, lo] + OPP[0]
            PB[2, hi] = PB[2, hi] + OPP[1]
        if s == NS - 1:
            for h in both:
                dw_part(XTD, h, s, end_ref, h)
            arrive(now)
            arrive(late)
            dx_ref[...] = (PB[3] + FULL[0] + FULL[1]).astype(dx_ref.dtype)
        for h in both:
            total(h, s).wait_recv()
            if s < NS - 1:
                dw_add(h, s)
        if s == 1:
            start(late)

    for s in range(NS):
        for h in both:
            gather(h, s).wait_send()
            forward(h, s).wait_send()
            total(h, s).wait_send()
    for copy in [w_swap, own_dy, x_swap] + x1 + x2a + x2b + x3i + x4i + x3ii + x4ii + x3iii + x4iii + opp + now + late:
        copy.wait_send()


def write(dx_ref, dw_ref, end_ref, dx_out, dw_out, last, sem):
    O = dw_ref.shape[1]
    SW = O // (2 * NS)
    copies = []

    def put(src, dst):
        copies.append(pltpu.make_async_copy(src, dst, sem.at[len(copies)]))
        copies[-1].start()

    tops = [(h + 1) * (O // 2) - SW for h in range(2)]
    for h in range(2):
        at = pl.ds(h * (O // 2), O // 2 - SW)
        put(dw_ref.at[:, at], dw_out.at[:, at])
    put(dx_ref, dx_out)
    for h in range(2):
        at = pl.ds(tops[h], SW)
        last[h] = dw_ref[:, at] + end_ref[h]
        put(last.at[h], dw_out.at[:, at])
    for copy in copies:
        copy.wait()


def solution(mesh):
    n, rows = mesh.shape["col"], mesh.shape["row"]
    assert n == 4 and mesh.shape["data"] == n and rows == 2
    act_spec = P(("pod", "data", "row"), "col")
    wgt_spec = P(("pod", "row"), "col")

    def local_step(x, w, dy):
        T, O = dy.shape
        F = x.shape[1]
        CT, FH = rows * T, F // rows
        QT, SW = CT // n, O // (2 * NS)
        bf16, f32 = jnp.bfloat16, jnp.float32
        dma = pltpu.SemaphoreType.DMA
        any_spec = pl.BlockSpec(memory_space=pl.ANY)
        vmem_spec = pl.BlockSpec(memory_space=pltpu.VMEM)
        dx, dw, end, _ = pl.pallas_call(
            functools.partial(kernel, n, rows),
            out_shape=[pltpu.VMEM((T, F), bf16), pltpu.VMEM((FH, O), f32), pltpu.VMEM((2, FH, SW), f32),
                       jax.ShapeDtypeStruct(w.shape, bf16)],
            in_specs=[any_spec] * 3,
            out_specs=[vmem_spec] * 3 + [any_spec],
            scratch_shapes=[
                pltpu.VMEM((2 * CT, O), bf16),
                pltpu.VMEM((CT, FH), bf16),
                pltpu.VMEM((n, QT, FH), bf16),
                pltpu.VMEM((7, n, QT, FH), bf16),
                pltpu.VMEM((2, FH, 2 * CT), bf16),
                pltpu.VMEM((2, FH, 2 * CT), bf16),
                pltpu.VMEM((2 * NS, FH, SW), f32),
                pltpu.VMEM((n, T, F), f32),
                pltpu.VMEM((2, T // 2, F), f32),
                pltpu.VMEM((2, T, F), f32),
                pltpu.VMEM((NW, F // NW, O), bf16),
                dma((2, NS)), dma((3,)), dma((2,)), dma((NW,)), dma((2,)),
                dma((2, NS)), dma((2, NS)), dma((2, NS)), dma((2, NS)),
                dma((n - 1,)), dma((n - 1,)), dma((4,)), dma((4,)), dma((18,)), dma((18,)),
                dma((6,)), dma((6,)), dma((2, NS)), dma((2, NS)),
            ],
            compiler_params=pltpu.CompilerParams(
                collective_id=0, has_side_effects=True, vmem_limit_bytes=56 * 1000 * 1000),
            cost_estimate=pl.CostEstimate(flops=16 * T * F * O * n // 4, bytes_accessed=4 * T * O, transcendentals=0),
        )(x, w, dy)
        dx, dw, end = [pltpu.with_memory_space_constraint(v, pltpu.VMEM) for v in (dx, dw, end)]
        return pl.pallas_call(
            write,
            out_shape=[jax.ShapeDtypeStruct((T, F), bf16), jax.ShapeDtypeStruct((FH, O), f32)],
            in_specs=[vmem_spec] * 3,
            out_specs=[any_spec] * 2,
            scratch_shapes=[pltpu.VMEM((2, FH, SW), f32), dma((5,))],
            compiler_params=pltpu.CompilerParams(vmem_limit_bytes=2 * 1000 * 1000),
        )(dx, dw, end)

    return jax.shard_map(local_step, mesh=mesh, in_specs=(act_spec, wgt_spec, act_spec), out_specs=(act_spec, act_spec),
                         check_vma=False)
```

```python
import functools

import jax
import jax.numpy as jnp
from jax import lax
from jax.experimental import pallas as pl
from jax.experimental.pallas import tpu as pltpu
from jax.sharding import PartitionSpec as P

MESH = pl.DeviceIdType.MESH
NS = 4
NW = 3


def kernel(n, rows, x_ref, w_ref, dy_ref, dx_ref, dw_ref, end_ref, ws_ref,
           DY, X0, X1, XA, XTP, XTD, RP, PB, OPP, FULL, WT,
           lsem, x0s, wx, wt, os, gs, gr, fs, fr, x1s, x1r, x2s, x2r, x3s, x3r, ps, pr, rs, rr):
    T, O = dy_ref.shape
    F = x_ref.shape[1]
    CT, TH, FH = rows * T, T // 2, F // rows
    QT, QH = CT // n, CT // n // 2
    SW, FT = O // (2 * NS), F // NW
    d, c, r = lax.axis_index("data"), lax.axis_index("col"), lax.axis_index("row")

    def mod(v):
        return lax.rem(v + 2 * n, n)

    cp, cm, sib = mod(c + 1), mod(c - 1), 1 - r
    pair = [d + 1 - 2 * lax.rem(d, 2), n - 1 - d]
    far = mod(d + 2)

    def remote(src, dst, ssem, rsem, **where):
        return pltpu.make_async_remote_copy(src_ref=src, dst_ref=dst, send_sem=ssem, recv_sem=rsem,
                                            device_id=where, device_id_type=MESH)

    def start(copies):
        for copy in copies:
            copy.start()

    def arrive(copies):
        for copy in copies:
            copy.wait_recv()

    mine = pl.ds(pl.multiple_of(r * T, T), T)
    other = pl.ds(pl.multiple_of(CT + r * T, T), T)

    def cols(h, s):
        return pl.ds(h * (O // 2) + s * SW, SW)

    def load_dy(h, s):
        return pltpu.make_async_copy(dy_ref.at[:, cols(h, s)], DY.at[mine, cols(h, s)], lsem.at[h, s])

    def gather(h, s):
        return remote(DY.at[mine, cols(h, s)], DY.at[other, cols(h, s)], gs.at[h, s], gr.at[h, s], data=pair[h])

    def forward(h, s):
        return remote(DY.at[other, cols(h, s)], DY.at[other, cols(h, s)], fs.at[h, s], fr.at[h, s], row=sib)

    own_dy = remote(DY.at[mine, :], DY.at[mine, :], os.at[0], os.at[1], row=sib)
    w_swap = remote(w_ref, ws_ref, wx.at[0], wx.at[1], row=sib)

    def feats(row):
        return pl.ds(pl.multiple_of(row * FH, FH), FH)

    x_keep = pltpu.make_async_copy(x_ref.at[:, feats(r)], X0.at[mine, :], x0s.at[0])
    x_swap = remote(x_ref.at[:, feats(sib)], X0.at[mine, :], x0s.at[1], x0s.at[2], row=sib)

    def quarter(j):
        return pl.ds(pl.multiple_of(j * QT, QT), QT)

    x1 = [remote(X0.at[quarter(mod(c + k)), :], X1.at[c], x1s.at[k - 1], x1r.at[k - 1], col=mod(c + k))
          for k in range(1, n)]
    x2a = [remote(X1.at[far], XA.at[2 + h, c], x2s.at[h], x2r.at[h], data=pair[h]) for h in range(2)]
    x2b = [remote(X1.at[pair[h]], XA.at[5 + h, c], x2s.at[2 + h], x2r.at[2 + h], data=pair[h]) for h in range(2)]

    slots = iter(range(64))

    def spread(src, dst):
        k, m = next(slots), next(slots)
        return [remote(src, dst, x3s.at[k], x3r.at[k], col=cp), remote(src, dst, x3s.at[m], x3r.at[m], col=cm)]

    def hand_on(right, left):
        k, m = next(slots), next(slots)
        return [remote(right, right, x3s.at[k], x3r.at[k], col=cp), remote(left, left, x3s.at[m], x3r.at[m], col=cm)]

    x3i = spread(X1.at[pair[1]], XA.at[0, c]) + spread(X1.at[pair[0]], XA.at[1, c])
    x4i = hand_on(XA.at[0, cm], XA.at[1, cp])
    x3ii = spread(XA.at[pl.ds(2, 2), c], XA.at[pl.ds(2, 2), c])
    x4ii = hand_on(XA.at[2, cm], XA.at[3, cp])
    x3iii = spread(X1.at[d], XA.at[4, c]) + spread(XA.at[pl.ds(5, 2), c], XA.at[pl.ds(5, 2), c])
    x4iii = (hand_on(XA.at[5, cm], XA.at[6, cp])
             + hand_on(XA.at[4, cm, pl.ds(0, QH)], XA.at[4, cp, pl.ds(QH, QH)]))

    lo, hi = pl.ds(0, TH), pl.ds(TH, TH)
    opp = [remote(PB.at[0, lo], OPP.at[0], ps.at[0], pr.at[0], col=cm),
           remote(PB.at[0, hi], OPP.at[1], ps.at[1], pr.at[1], col=cp)]
    now = [remote(PB.at[1, hi], FULL.at[0, hi], ps.at[2], pr.at[2], col=cm),
           remote(PB.at[2, lo], FULL.at[1, lo], ps.at[3], pr.at[3], col=cp)]
    late = [remote(PB.at[1, lo], FULL.at[0, lo], ps.at[4], pr.at[4], col=cm),
            remote(PB.at[2, hi], FULL.at[1, hi], ps.at[5], pr.at[5], col=cp)]

    def total(h, s):
        return remote(RP.at[h * NS + s], dw_ref.at[:, cols(h, s)], rs.at[h, s], rr.at[h, s], data=pair[1 - h])

    target = [mod(c + 2), cm, cp, c]
    per = n // rows

    def tile_wait(i):
        pltpu.make_async_copy(w_ref.at[pl.ds(0, FT), :], WT.at[i], wt.at[i]).wait()

    def tile_start(k, i):
        b = target[k]
        row0 = pl.multiple_of(lax.rem(b, per) * F + i * FT, FT)

        @pl.when(b // per == r)
        def _():
            pltpu.make_async_copy(w_ref.at[pl.ds(row0, FT), :], WT.at[i], wt.at[i]).start()

        @pl.when(b // per != r)
        def _():
            pltpu.make_async_copy(ws_ref.at[pl.ds(row0, FT), :], WT.at[i], wt.at[i]).start()

    def dx_block(k):
        def one(i, carry):
            tile_wait(i)
            PB[k, :, pl.ds(pl.multiple_of(i * FT, FT), FT)] = lax.dot_general(
                DY[mine, :], WT[i], (((1,), (1,)), ((), ())), preferred_element_type=jnp.float32)
            if k + 1 < n:
                tile_start(k + 1, i)
            return carry

        lax.fori_loop(0, NW, one, 0)

    half = SW // 2

    def product(xt, h, s, i):
        return lax.dot_general(xt, DY[:, pl.ds(pl.multiple_of(h * (O // 2) + s * SW + i * half, half), half)],
                               (((1,), (0,)), ((), ())), preferred_element_type=jnp.float32)

    def dw_part(xt, h, s, out, slot):
        def one(i, carry):
            out[slot, :, pl.ds(pl.multiple_of(i * half, half), half)] = product(xt[h], h, s, i)
            return carry

        lax.fori_loop(0, 2, one, 0)

    def dw_add(h, s):
        def one(i, carry):
            at = pl.ds(pl.multiple_of(h * (O // 2) + s * SW + i * half, half), half)
            dw_ref[:, at] = dw_ref[:, at] + product(XTD[h], h, s, i)
            return carry

        lax.fori_loop(0, 2, one, 0)

    def turn(block, places):
        for j in range(n):
            value = XA[block, j].T
            for ref, h, side in places:
                ref[h, :, pl.ds(side * CT + j * QT, QT)] = value

    both = range(2)
    for s in range(NS):
        for h in both:
            load_dy(h, s).start()
    x_keep.start()
    barrier = pltpu.get_barrier_semaphore()
    peers = [{"row": sib}] + [{"data": p} for p in pair] + [{"col": mod(c + k)} for k in range(1, n)]
    for peer in peers:
        pl.semaphore_signal(barrier, inc=1, device_id=peer, device_id_type=MESH)
    pl.semaphore_wait(barrier, len(peers))

    x_swap.start()
    for s in range(2):
        for h in both:
            load_dy(h, s).wait()

    first = r == 1

    @pl.when(first)
    def _():
        for s in range(2):
            for h in both:
                gather(h, s).start()

    w_swap.start()
    x_keep.wait()
    x_swap.wait_recv()

    @pl.when(jnp.logical_not(first))
    def _():
        for s in range(2):
            for h in both:
                gather(h, s).start()

    start(x1)
    X1[c] = X0[quarter(c), :]
    for s in range(2, NS):
        for h in both:
            load_dy(h, s).wait()
    own_dy.start()
    arrive(x1)
    start(x3i)
    start(x2a)
    start(x2b)
    for s in range(2, NS):
        for h in both:
            gather(h, s).start()
    XA[0, c] = X1[pair[1]]
    XA[1, c] = X1[pair[0]]
    XA[4, c] = X1[d]
    for h in both:
        gather(h, 0).wait_recv()
        forward(h, 0).start()
    arrive(x2a)
    start(x3ii)
    arrive(x3i)
    start(x4i)
    w_swap.wait_recv()
    for i in range(NW):
        tile_start(0, i)
    dx_block(0)
    for h in both:
        gather(h, 1).wait_recv()
        forward(h, 1).start()
    arrive(x3ii)
    start(x4ii)
    dx_block(1)
    arrive(x2b)
    start(x3iii)
    dx_block(2)
    arrive(x4i)
    turn(0, [(XTP, 0, 0)])
    turn(1, [(XTP, 1, 0)])
    arrive(x4ii)
    turn(2, [(XTP, 0, 1)])
    turn(3, [(XTP, 1, 1)])
    own_dy.wait_recv()
    for s in range(NS):
        if s + 2 < NS:
            for h in both:
                gather(h, s + 2).wait_recv()
                forward(h, s + 2).start()
        for h in both:
            forward(h, s).wait_recv()
            dw_part(XTP, h, s, RP, h * NS + s)
        if s == 1:
            arrive(x3iii)
            start(x4iii)
            start(opp)
            start(now)
        for h in both:
            total(h, s).start()
    dx_block(3)
    arrive(x4iii)
    turn(4, [(XTD, 0, 0), (XTD, 1, 0)])
    turn(5, [(XTD, 0, 1)])
    turn(6, [(XTD, 1, 1)])
    for s in range(NS):
        if s == 1:
            arrive(opp)
            PB[1, lo] = PB[1, lo] + OPP[0]
            PB[2, hi] = PB[2, hi] + OPP[1]
        if s == NS - 1:
            for h in both:
                dw_part(XTD, h, s, end_ref, h)
            arrive(now)
            arrive(late)
            dx_ref[...] = (PB[3] + FULL[0] + FULL[1]).astype(dx_ref.dtype)
        for h in both:
            total(h, s).wait_recv()
            if s < NS - 1:
                dw_add(h, s)
        if s == 1:
            start(late)

    for s in range(NS):
        for h in both:
            gather(h, s).wait_send()
            forward(h, s).wait_send()
            total(h, s).wait_send()
    for copy in [w_swap, own_dy, x_swap] + x1 + x2a + x2b + x3i + x4i + x3ii + x4ii + x3iii + x4iii + opp + now + late:
        copy.wait_send()


def write(dx_ref, dw_ref, end_ref, dx_out, dw_out, last, sem):
    O = dw_ref.shape[1]
    SW = O // (2 * NS)
    copies = []

    def put(src, dst):
        copies.append(pltpu.make_async_copy(src, dst, sem.at[len(copies)]))
        copies[-1].start()

    tops = [(h + 1) * (O // 2) - SW for h in range(2)]
    for h in range(2):
        at = pl.ds(h * (O // 2), O // 2 - SW)
        put(dw_ref.at[:, at], dw_out.at[:, at])
    put(dx_ref, dx_out)
    for h in range(2):
        at = pl.ds(tops[h], SW)
        last[h] = dw_ref[:, at] + end_ref[h]
        put(last.at[h], dw_out.at[:, at])
    for copy in copies:
        copy.wait()


def solution(mesh):
    n, rows = mesh.shape["col"], mesh.shape["row"]
    assert n == 4 and mesh.shape["data"] == n and rows == 2
    act_spec = P(("pod", "data", "row"), "col")
    wgt_spec = P(("pod", "row"), "col")

    def local_step(x, w, dy):
        T, O = dy.shape
        F = x.shape[1]
        CT, FH = rows * T, F // rows
        QT, SW = CT // n, O // (2 * NS)
        bf16, f32 = jnp.bfloat16, jnp.float32
        dma = pltpu.SemaphoreType.DMA
        any_spec = pl.BlockSpec(memory_space=pl.ANY)
        vmem_spec = pl.BlockSpec(memory_space=pltpu.VMEM)
        dx, dw, end, _ = pl.pallas_call(
            functools.partial(kernel, n, rows),
            out_shape=[pltpu.VMEM((T, F), bf16), pltpu.VMEM((FH, O), f32), pltpu.VMEM((2, FH, SW), f32),
                       jax.ShapeDtypeStruct(w.shape, bf16)],
            in_specs=[any_spec] * 3,
            out_specs=[vmem_spec] * 3 + [any_spec],
            scratch_shapes=[
                pltpu.VMEM((2 * CT, O), bf16),
                pltpu.VMEM((CT, FH), bf16),
                pltpu.VMEM((n, QT, FH), bf16),
                pltpu.VMEM((7, n, QT, FH), bf16),
                pltpu.VMEM((2, FH, 2 * CT), bf16),
                pltpu.VMEM((2, FH, 2 * CT), bf16),
                pltpu.VMEM((2 * NS, FH, SW), f32),
                pltpu.VMEM((n, T, F), f32),
                pltpu.VMEM((2, T // 2, F), f32),
                pltpu.VMEM((2, T, F), f32),
                pltpu.VMEM((NW, F // NW, O), bf16),
                dma((2, NS)), dma((3,)), dma((2,)), dma((NW,)), dma((2,)),
                dma((2, NS)), dma((2, NS)), dma((2, NS)), dma((2, NS)),
                dma((n - 1,)), dma((n - 1,)), dma((4,)), dma((4,)), dma((18,)), dma((18,)),
                dma((6,)), dma((6,)), dma((2, NS)), dma((2, NS)),
            ],
            compiler_params=pltpu.CompilerParams(
                collective_id=0, has_side_effects=True, vmem_limit_bytes=56 * 1000 * 1000),
            cost_estimate=pl.CostEstimate(flops=16 * T * F * O * n // 4, bytes_accessed=4 * T * O, transcendentals=0),
        )(x, w, dy)
        dx, dw, end = [pltpu.with_memory_space_constraint(v, pltpu.VMEM) for v in (dx, dw, end)]
        return pl.pallas_call(
            write,
            out_shape=[jax.ShapeDtypeStruct((T, F), bf16), jax.ShapeDtypeStruct((FH, O), f32)],
            in_specs=[vmem_spec] * 3,
            out_specs=[any_spec] * 2,
            scratch_shapes=[pltpu.VMEM((2, FH, SW), f32), dma((5,))],
            compiler_params=pltpu.CompilerParams(vmem_limit_bytes=2 * 1000 * 1000),
        )(dx, dw, end)

    return jax.shard_map(local_step, mesh=mesh, in_specs=(act_spec, wgt_spec, act_spec), out_specs=(act_spec, act_spec),
                         check_vma=False)
```

```python
import functools

import jax
import jax.numpy as jnp
from jax import lax
from jax.experimental import pallas as pl
from jax.experimental.pallas import tpu as pltpu
from jax.sharding import PartitionSpec as P

MESH = pl.DeviceIdType.MESH
NS = 4
NW = 3


def kernel(n, rows, x_ref, w_ref, dy_ref, dx_ref, dw_ref, end_ref, ws_ref,
           DY, X0, X1, XA, XTP, XTD, RP, PB, OPP, FULL, WT,
           lsem, x0s, wx, wt, os, gs, gr, fs, fr, x1s, x1r, x2s, x2r, x3s, x3r, ps, pr, rs, rr, there):
    T, O = dy_ref.shape
    F = x_ref.shape[1]
    CT, TH, FH = rows * T, T // 2, F // rows
    QT, QH = CT // n, CT // n // 2
    SW, FT = O // (2 * NS), F // NW
    d, c, r = lax.axis_index("data"), lax.axis_index("col"), lax.axis_index("row")

    def mod(v):
        return lax.rem(v + 2 * n, n)

    cp, cm, sib = mod(c + 1), mod(c - 1), 1 - r
    pair = [d + 1 - 2 * lax.rem(d, 2), n - 1 - d]
    far = mod(d + 2)

    def remote(src, dst, ssem, rsem, **where):
        return pltpu.make_async_remote_copy(src_ref=src, dst_ref=dst, send_sem=ssem, recv_sem=rsem,
                                            device_id=where, device_id_type=MESH)

    def start(copies):
        for copy in copies:
            copy.start()

    def arrive(copies):
        for copy in copies:
            copy.wait_recv()

    mine = pl.ds(pl.multiple_of(r * T, T), T)
    other = pl.ds(pl.multiple_of(CT + r * T, T), T)

    def cols(h, s):
        return pl.ds(h * (O // 2) + s * SW, SW)

    def load_dy(h, s):
        return pltpu.make_async_copy(dy_ref.at[:, cols(h, s)], DY.at[mine, cols(h, s)], lsem.at[h, s])

    def gather(h, s):
        return remote(dy_ref.at[:, cols(h, s)], DY.at[other, cols(h, s)], gs.at[h, s], gr.at[h, s], data=pair[h])

    def forward(h, s):
        return remote(DY.at[other, cols(h, s)], DY.at[other, cols(h, s)], fs.at[h, s], fr.at[h, s], row=sib)

    own_dy = remote(DY.at[mine, :], DY.at[mine, :], os.at[0], os.at[1], row=sib)
    w_swap = remote(w_ref, ws_ref, wx.at[0], wx.at[1], row=sib)

    def feats(row):
        return pl.ds(pl.multiple_of(row * FH, FH), FH)

    x_keep = pltpu.make_async_copy(x_ref.at[:, feats(r)], X0.at[mine, :], x0s.at[0])
    x_swap = remote(x_ref.at[:, feats(sib)], X0.at[mine, :], x0s.at[1], x0s.at[2], row=sib)

    def quarter(j):
        return pl.ds(pl.multiple_of(j * QT, QT), QT)

    x1 = [remote(X0.at[quarter(mod(c + k)), :], X1.at[c], x1s.at[k - 1], x1r.at[k - 1], col=mod(c + k))
          for k in range(1, n)]
    x2a = [remote(X1.at[far], XA.at[2 + h, c], x2s.at[h], x2r.at[h], data=pair[h]) for h in range(2)]
    x2b = [remote(X1.at[pair[h]], XA.at[5 + h, c], x2s.at[2 + h], x2r.at[2 + h], data=pair[h]) for h in range(2)]

    slots = iter(range(64))

    def spread(src, dst):
        k, m = next(slots), next(slots)
        return [remote(src, dst, x3s.at[k], x3r.at[k], col=cp), remote(src, dst, x3s.at[m], x3r.at[m], col=cm)]

    def hand_on(right, left):
        k, m = next(slots), next(slots)
        return [remote(right, right, x3s.at[k], x3r.at[k], col=cp), remote(left, left, x3s.at[m], x3r.at[m], col=cm)]

    x3i = spread(X1.at[pair[1]], XA.at[0, c]) + spread(X1.at[pair[0]], XA.at[1, c])
    x4i = hand_on(XA.at[0, cm], XA.at[1, cp])
    x3ii = spread(XA.at[pl.ds(2, 2), c], XA.at[pl.ds(2, 2), c])
    x4ii = hand_on(XA.at[2, cm], XA.at[3, cp])
    x3iii = spread(X1.at[d], XA.at[4, c]) + spread(XA.at[pl.ds(5, 2), c], XA.at[pl.ds(5, 2), c])
    x4iii = (hand_on(XA.at[5, cm], XA.at[6, cp])
             + hand_on(XA.at[4, cm, pl.ds(0, QH)], XA.at[4, cp, pl.ds(QH, QH)]))

    lo, hi = pl.ds(0, TH), pl.ds(TH, TH)
    opp = [remote(PB.at[0, lo], OPP.at[0], ps.at[0], pr.at[0], col=cm),
           remote(PB.at[0, hi], OPP.at[1], ps.at[1], pr.at[1], col=cp)]
    now = [remote(PB.at[1, hi], FULL.at[0, hi], ps.at[2], pr.at[2], col=cm),
           remote(PB.at[2, lo], FULL.at[1, lo], ps.at[3], pr.at[3], col=cp)]
    late = [remote(PB.at[1, lo], FULL.at[0, lo], ps.at[4], pr.at[4], col=cm),
            remote(PB.at[2, hi], FULL.at[1, hi], ps.at[5], pr.at[5], col=cp)]

    def total(h, s):
        return remote(RP.at[h * NS + s], dw_ref.at[:, cols(h, s)], rs.at[h, s], rr.at[h, s], data=pair[1 - h])

    target = [mod(c + 2), cm, cp, c]
    per = n // rows

    def tile_wait(i):
        pltpu.make_async_copy(w_ref.at[pl.ds(0, FT), :], WT.at[i], wt.at[i]).wait()

    def tile_start(k, i):
        b = target[k]
        row0 = pl.multiple_of(lax.rem(b, per) * F + i * FT, FT)

        @pl.when(b // per == r)
        def _():
            pltpu.make_async_copy(w_ref.at[pl.ds(row0, FT), :], WT.at[i], wt.at[i]).start()

        @pl.when(b // per != r)
        def _():
            pltpu.make_async_copy(ws_ref.at[pl.ds(row0, FT), :], WT.at[i], wt.at[i]).start()

    def dx_block(k):
        def one(i, carry):
            tile_wait(i)
            PB[k, :, pl.ds(pl.multiple_of(i * FT, FT), FT)] = lax.dot_general(
                DY[mine, :], WT[i], (((1,), (1,)), ((), ())), preferred_element_type=jnp.float32)
            if k + 1 < n:
                tile_start(k + 1, i)
            return carry

        lax.fori_loop(0, NW, one, 0)

    half = SW // 2

    def product(xt, h, s, i):
        return lax.dot_general(xt, DY[:, pl.ds(pl.multiple_of(h * (O // 2) + s * SW + i * half, half), half)],
                               (((1,), (0,)), ((), ())), preferred_element_type=jnp.float32)

    def dw_part(xt, h, s, out, slot):
        def one(i, carry):
            out[slot, :, pl.ds(pl.multiple_of(i * half, half), half)] = product(xt[h], h, s, i)
            return carry

        lax.fori_loop(0, 2, one, 0)

    def dw_add(h, s):
        def one(i, carry):
            at = pl.ds(pl.multiple_of(h * (O // 2) + s * SW + i * half, half), half)
            dw_ref[:, at] = dw_ref[:, at] + product(XTD[h], h, s, i)
            return carry

        lax.fori_loop(0, 2, one, 0)

    def turn(block, places):
        for j in range(n):
            value = XA[block, j].T
            for ref, h, side in places:
                ref[h, :, pl.ds(side * CT + j * QT, QT)] = value

    both = range(2)
    barrier = pltpu.get_barrier_semaphore()
    early = r == 1

    def greet(**where):
        pl.semaphore_signal(barrier, inc=1, device_id=where, device_id_type=MESH)

    for p in pair:
        greet(data=p)


    @pl.when(early)
    def _():
        greet(row=sib)
        for k in range(1, n):
            greet(col=mod(c + k), row=sib)
        pl.semaphore_wait(barrier, 2)

    @pl.when(jnp.logical_not(early))
    def _():
        for k in range(1, n):
            greet(col=mod(c + k))
        pl.semaphore_wait(barrier, 2 + 1 + 2 * (n - 1))
        pl.semaphore_signal(there, inc=1, device_id={"row": sib}, device_id_type=MESH)


    for s in range(2):
        for h in both:
            gather(h, s).start()
    for s in range(NS):
        for h in both:
            load_dy(h, s).start()
    x_keep.start()

    @pl.when(early)
    def _():
        pl.semaphore_wait(there, 1)

    x_swap.start()
    w_swap.start()
    x_keep.wait()
    x_swap.wait_recv()

    start(x1)
    X1[c] = X0[quarter(c), :]
    for s in range(NS):
        for h in both:
            load_dy(h, s).wait()
    own_dy.start()
    arrive(x1)
    start(x3i)
    start(x2a)
    start(x2b)
    for s in range(2, NS):
        for h in both:
            gather(h, s).start()
    XA[0, c] = X1[pair[1]]
    XA[1, c] = X1[pair[0]]
    XA[4, c] = X1[d]
    for h in both:
        gather(h, 0).wait_recv()
        forward(h, 0).start()
    arrive(x2a)
    start(x3ii)
    arrive(x3i)
    start(x4i)
    w_swap.wait_recv()
    for i in range(NW):
        tile_start(0, i)
    dx_block(0)
    for h in both:
        gather(h, 1).wait_recv()
        forward(h, 1).start()
    arrive(x3ii)
    start(x4ii)
    dx_block(1)
    arrive(x2b)
    start(x3iii)
    dx_block(2)
    arrive(x4i)
    turn(0, [(XTP, 0, 0)])
    turn(1, [(XTP, 1, 0)])
    arrive(x4ii)
    turn(2, [(XTP, 0, 1)])
    turn(3, [(XTP, 1, 1)])
    own_dy.wait_recv()
    for s in range(NS):
        if s + 2 < NS:
            for h in both:
                gather(h, s + 2).wait_recv()
                forward(h, s + 2).start()
        for h in both:
            forward(h, s).wait_recv()
            dw_part(XTP, h, s, RP, h * NS + s)
        if s == 1:
            arrive(x3iii)
            start(x4iii)
            start(opp)
            start(now)
        for h in both:
            total(h, s).start()
    dx_block(3)
    arrive(x4iii)
    turn(4, [(XTD, 0, 0), (XTD, 1, 0)])
    turn(5, [(XTD, 0, 1)])
    turn(6, [(XTD, 1, 1)])
    for s in range(NS):
        if s == 1:
            arrive(opp)
            PB[1, lo] = PB[1, lo] + OPP[0]
            PB[2, hi] = PB[2, hi] + OPP[1]
        if s == NS - 1:
            for h in both:
                dw_part(XTD, h, s, end_ref, h)
            arrive(now)
            arrive(late)
            dx_ref[...] = (PB[3] + FULL[0] + FULL[1]).astype(dx_ref.dtype)
        for h in both:
            if s < NS - 1:
                total(h, s).wait_recv()
                dw_add(h, s)
        if s == 1:
            start(late)

    for s in range(NS):
        for h in both:
            gather(h, s).wait_send()
            forward(h, s).wait_send()
            if s < NS - 1:
                total(h, s).wait_send()
    for copy in [w_swap, own_dy, x_swap] + x1 + x2a + x2b + x3i + x4i + x3ii + x4ii + x3iii + x4iii + opp + now + late:
        copy.wait_send()
    for h in both:
        total(h, NS - 1).wait()


def write(dx_ref, dw_ref, end_ref, dx_out, dw_out, last, sem):
    O = dw_ref.shape[1]
    SW = O // (2 * NS)
    copies = []

    def put(src, dst):
        copies.append(pltpu.make_async_copy(src, dst, sem.at[len(copies)]))
        copies[-1].start()

    tops = [(h + 1) * (O // 2) - SW for h in range(2)]
    for h in range(2):
        at = pl.ds(h * (O // 2), O // 2 - SW)
        put(dw_ref.at[:, at], dw_out.at[:, at])
    put(dx_ref, dx_out)
    for h in range(2):
        at = pl.ds(tops[h], SW)
        last[h] = dw_ref[:, at] + end_ref[h]
        put(last.at[h], dw_out.at[:, at])
    for copy in copies:
        copy.wait()


def solution(mesh):
    n, rows = mesh.shape["col"], mesh.shape["row"]
    assert n == 4 and mesh.shape["data"] == n and rows == 2
    act_spec = P(("pod", "data", "row"), "col")
    wgt_spec = P(("pod", "row"), "col")

    def local_step(x, w, dy):
        T, O = dy.shape
        F = x.shape[1]
        CT, FH = rows * T, F // rows
        QT, SW = CT // n, O // (2 * NS)
        bf16, f32 = jnp.bfloat16, jnp.float32
        dma = pltpu.SemaphoreType.DMA
        any_spec = pl.BlockSpec(memory_space=pl.ANY)
        vmem_spec = pl.BlockSpec(memory_space=pltpu.VMEM)
        dx, dw, end, _ = pl.pallas_call(
            functools.partial(kernel, n, rows),
            out_shape=[pltpu.VMEM((T, F), bf16), pltpu.VMEM((FH, O), f32), pltpu.VMEM((2, FH, SW), f32),
                       jax.ShapeDtypeStruct(w.shape, bf16)],
            in_specs=[any_spec] * 3,
            out_specs=[vmem_spec] * 3 + [any_spec],
            scratch_shapes=[
                pltpu.VMEM((2 * CT, O), bf16),
                pltpu.VMEM((CT, FH), bf16),
                pltpu.VMEM((n, QT, FH), bf16),
                pltpu.VMEM((7, n, QT, FH), bf16),
                pltpu.VMEM((2, FH, 2 * CT), bf16),
                pltpu.VMEM((2, FH, 2 * CT), bf16),
                pltpu.VMEM((2 * NS, FH, SW), f32),
                pltpu.VMEM((n, T, F), f32),
                pltpu.VMEM((2, T // 2, F), f32),
                pltpu.VMEM((2, T, F), f32),
                pltpu.VMEM((NW, F // NW, O), bf16),
                dma((2, NS)), dma((3,)), dma((2,)), dma((NW,)), dma((2,)),
                dma((2, NS)), dma((2, NS)), dma((2, NS)), dma((2, NS)),
                dma((n - 1,)), dma((n - 1,)), dma((4,)), dma((4,)), dma((18,)), dma((18,)),
                dma((6,)), dma((6,)), dma((2, NS)), dma((2, NS)), pltpu.SemaphoreType.REGULAR,
            ],
            compiler_params=pltpu.CompilerParams(
                collective_id=0, has_side_effects=True, vmem_limit_bytes=56 * 1000 * 1000),
            cost_estimate=pl.CostEstimate(flops=16 * T * F * O * n // 4, bytes_accessed=4 * T * O, transcendentals=0),
        )(x, w, dy)
        dx, dw, end = [pltpu.with_memory_space_constraint(v, pltpu.VMEM) for v in (dx, dw, end)]
        return pl.pallas_call(
            write,
            out_shape=[jax.ShapeDtypeStruct((T, F), bf16), jax.ShapeDtypeStruct((FH, O), f32)],
            in_specs=[vmem_spec] * 3,
            out_specs=[any_spec] * 2,
            scratch_shapes=[pltpu.VMEM((2, FH, SW), f32), dma((5,))],
            compiler_params=pltpu.CompilerParams(vmem_limit_bytes=2 * 1000 * 1000),
        )(dx, dw, end)

    return jax.shard_map(local_step, mesh=mesh, in_specs=(act_spec, wgt_spec, act_spec), out_specs=(act_spec, act_spec),
                         check_vma=False)
```

```python
import functools

import jax
import jax.numpy as jnp
from jax import lax
from jax.experimental import pallas as pl
from jax.experimental.pallas import tpu as pltpu
from jax.sharding import PartitionSpec as P

MESH = pl.DeviceIdType.MESH
NS = 4
NW = 3


def kernel(n, rows, x_ref, w_ref, dy_ref, dx_ref, dw_ref, end_ref, ws_ref,
           DY, X0, X1, XA, XTP, XTD, RP, PB, OPP, FULL, WT,
           lsem, x0s, wx, wt, os, gs, gr, fs, fr, x1s, x1r, x2s, x2r, x3s, x3r, ps, pr, rs, rr, there):
    T, O = dy_ref.shape
    F = x_ref.shape[1]
    CT, TH, FH = rows * T, T // 2, F // rows
    QT, QH = CT // n, CT // n // 2
    SW, FT = O // (2 * NS), F // NW
    d, c, r = lax.axis_index("data"), lax.axis_index("col"), lax.axis_index("row")

    def mod(v):
        return lax.rem(v + 2 * n, n)

    cp, cm, sib = mod(c + 1), mod(c - 1), 1 - r
    pair = [d + 1 - 2 * lax.rem(d, 2), n - 1 - d]
    far = mod(d + 2)

    def remote(src, dst, ssem, rsem, **where):
        return pltpu.make_async_remote_copy(src_ref=src, dst_ref=dst, send_sem=ssem, recv_sem=rsem,
                                            device_id=where, device_id_type=MESH)

    def start(copies):
        for copy in copies:
            copy.start()

    def arrive(copies):
        for copy in copies:
            copy.wait_recv()

    mine = pl.ds(pl.multiple_of(r * T, T), T)
    other = pl.ds(pl.multiple_of(CT + r * T, T), T)

    def cols(h, s):
        return pl.ds(h * (O // 2) + s * SW, SW)

    load_dy = pltpu.make_async_copy(dy_ref, DY.at[mine, :], lsem)

    def gather(h, s):
        return remote(dy_ref.at[:, cols(h, s)], DY.at[other, cols(h, s)], gs.at[h, s], gr.at[h, s], data=pair[h])

    def forward(h, s):
        return remote(DY.at[other, cols(h, s)], DY.at[other, cols(h, s)], fs.at[h, s], fr.at[h, s], row=sib)

    own_dy = remote(dy_ref, DY.at[mine, :], os.at[0], os.at[1], row=sib)
    w_swap = remote(w_ref, ws_ref, wx.at[0], wx.at[1], row=sib)

    def feats(row):
        return pl.ds(pl.multiple_of(row * FH, FH), FH)

    x_keep = pltpu.make_async_copy(x_ref.at[:, feats(r)], X0.at[mine, :], x0s.at[0])
    x_swap = remote(x_ref.at[:, feats(sib)], X0.at[mine, :], x0s.at[1], x0s.at[2], row=sib)

    def quarter(j):
        return pl.ds(pl.multiple_of(j * QT, QT), QT)

    x1 = [remote(X0.at[quarter(mod(c + k)), :], X1.at[c], x1s.at[k - 1], x1r.at[k - 1], col=mod(c + k))
          for k in range(1, n)]
    x2a = [remote(X1.at[far], XA.at[2 + h, c], x2s.at[h], x2r.at[h], data=pair[h]) for h in range(2)]
    x2b = [remote(X1.at[pair[h]], XA.at[5 + h, c], x2s.at[2 + h], x2r.at[2 + h], data=pair[h]) for h in range(2)]

    slots = iter(range(64))

    def spread(src, dst):
        k, m = next(slots), next(slots)
        return [remote(src, dst, x3s.at[k], x3r.at[k], col=cp), remote(src, dst, x3s.at[m], x3r.at[m], col=cm)]

    def hand_on(right, left):
        k, m = next(slots), next(slots)
        return [remote(right, right, x3s.at[k], x3r.at[k], col=cp), remote(left, left, x3s.at[m], x3r.at[m], col=cm)]

    x3i = spread(X1.at[pair[1]], XA.at[0, c]) + spread(X1.at[pair[0]], XA.at[1, c])
    x4i = hand_on(XA.at[0, cm], XA.at[1, cp])
    x3ii = spread(XA.at[pl.ds(2, 2), c], XA.at[pl.ds(2, 2), c])
    x4ii = hand_on(XA.at[2, cm], XA.at[3, cp])
    x3iii = spread(X1.at[d], XA.at[4, c]) + spread(XA.at[pl.ds(5, 2), c], XA.at[pl.ds(5, 2), c])
    x4iii = (hand_on(XA.at[5, cm], XA.at[6, cp])
             + hand_on(XA.at[4, cm, pl.ds(0, QH)], XA.at[4, cp, pl.ds(QH, QH)]))

    lo, hi = pl.ds(0, TH), pl.ds(TH, TH)
    opp = [remote(PB.at[0, lo], OPP.at[0], ps.at[0], pr.at[0], col=cm),
           remote(PB.at[0, hi], OPP.at[1], ps.at[1], pr.at[1], col=cp)]
    now = [remote(PB.at[1, hi], FULL.at[0, hi], ps.at[2], pr.at[2], col=cm),
           remote(PB.at[2, lo], FULL.at[1, lo], ps.at[3], pr.at[3], col=cp)]
    late = [remote(PB.at[1, lo], FULL.at[0, lo], ps.at[4], pr.at[4], col=cm),
            remote(PB.at[2, hi], FULL.at[1, hi], ps.at[5], pr.at[5], col=cp)]

    def total(h, s):
        return remote(RP.at[h * NS + s], dw_ref.at[:, cols(h, s)], rs.at[h, s], rr.at[h, s], data=pair[1 - h])

    target = [mod(c + 2), cm, cp, c]
    per = n // rows

    def tile_wait(i):
        pltpu.make_async_copy(w_ref.at[pl.ds(0, FT), :], WT.at[i], wt.at[i]).wait()

    def tile_start(k, i):
        b = target[k]
        row0 = pl.multiple_of(lax.rem(b, per) * F + i * FT, FT)

        @pl.when(b // per == r)
        def _():
            pltpu.make_async_copy(w_ref.at[pl.ds(row0, FT), :], WT.at[i], wt.at[i]).start()

        @pl.when(b // per != r)
        def _():
            pltpu.make_async_copy(ws_ref.at[pl.ds(row0, FT), :], WT.at[i], wt.at[i]).start()

    def dx_block(k):
        def one(i, carry):
            tile_wait(i)
            PB[k, :, pl.ds(pl.multiple_of(i * FT, FT), FT)] = lax.dot_general(
                DY[mine, :], WT[i], (((1,), (1,)), ((), ())), preferred_element_type=jnp.float32)
            if k + 1 < n:
                tile_start(k + 1, i)
            return carry

        lax.fori_loop(0, NW, one, 0)

    half = SW // 2

    def product(xt, h, s, i):
        return lax.dot_general(xt, DY[:, pl.ds(pl.multiple_of(h * (O // 2) + s * SW + i * half, half), half)],
                               (((1,), (0,)), ((), ())), preferred_element_type=jnp.float32)

    def dw_part(xt, h, s, out, slot):
        def one(i, carry):
            out[slot, :, pl.ds(pl.multiple_of(i * half, half), half)] = product(xt[h], h, s, i)
            return carry

        lax.fori_loop(0, 2, one, 0)

    def dw_add(h, s):
        def one(i, carry):
            at = pl.ds(pl.multiple_of(h * (O // 2) + s * SW + i * half, half), half)
            dw_ref[:, at] = dw_ref[:, at] + product(XTD[h], h, s, i)
            return carry

        lax.fori_loop(0, 2, one, 0)

    def turn(block, places):
        for j in range(n):
            value = XA[block, j].T
            for ref, h, side in places:
                ref[h, :, pl.ds(side * CT + j * QT, QT)] = value

    both = range(2)
    barrier = pltpu.get_barrier_semaphore()
    early = r == 1

    def greet(**where):
        pl.semaphore_signal(barrier, inc=1, device_id=where, device_id_type=MESH)

    for p in pair:
        greet(data=p)


    @pl.when(early)
    def _():
        pl.semaphore_wait(barrier, 2)
        for h in both:
            gather(h, 0).start()
        greet(row=sib)
        for k in range(1, n):
            greet(col=mod(c + k), row=sib)

    @pl.when(jnp.logical_not(early))
    def _():
        for k in range(1, n):
            greet(col=mod(c + k))
        pl.semaphore_wait(barrier, 2 + 1 + 2 * (n - 1))
        pl.semaphore_signal(there, inc=1, device_id={"row": sib}, device_id_type=MESH)


    @pl.when(jnp.logical_not(early))
    def _():
        for h in both:
            gather(h, 0).start()

    for h in both:
        gather(h, 1).start()
    load_dy.start()
    x_keep.start()

    @pl.when(early)
    def _():
        pl.semaphore_wait(there, 1)

    x_swap.start()
    w_swap.start()
    x_keep.wait()
    x_swap.wait_recv()

    start(x1)
    X1[c] = X0[quarter(c), :]
    own_dy.start()
    arrive(x1)
    start(x3i)
    start(x2a)
    start(x2b)
    for s in range(2, NS):
        for h in both:
            gather(h, s).start()
    XA[0, c] = X1[pair[1]]
    XA[1, c] = X1[pair[0]]
    XA[4, c] = X1[d]
    for h in both:
        gather(h, 0).wait_recv()
        forward(h, 0).start()
    arrive(x2a)
    start(x3ii)
    arrive(x3i)
    start(x4i)
    load_dy.wait()
    w_swap.wait_recv()
    for i in range(NW):
        tile_start(0, i)
    dx_block(0)
    for h in both:
        gather(h, 1).wait_recv()
        forward(h, 1).start()
    arrive(x3ii)
    start(x4ii)
    dx_block(1)
    arrive(x2b)
    start(x3iii)
    dx_block(2)
    arrive(x4i)
    turn(0, [(XTP, 0, 0)])
    turn(1, [(XTP, 1, 0)])
    arrive(x4ii)
    turn(2, [(XTP, 0, 1)])
    turn(3, [(XTP, 1, 1)])
    own_dy.wait_recv()
    for s in range(NS):
        if s + 2 < NS:
            for h in both:
                gather(h, s + 2).wait_recv()
                forward(h, s + 2).start()
        for h in both:
            forward(h, s).wait_recv()
            dw_part(XTP, h, s, RP, h * NS + s)
        if s == 1:
            arrive(x3iii)
            start(x4iii)
            start(opp)
            start(now)
        for h in both:
            total(h, s).start()
    dx_block(3)
    arrive(x4iii)
    turn(4, [(XTD, 0, 0), (XTD, 1, 0)])
    turn(5, [(XTD, 0, 1)])
    turn(6, [(XTD, 1, 1)])
    for s in range(NS):
        if s == 1:
            arrive(opp)
            PB[1, lo] = PB[1, lo] + OPP[0]
            PB[2, hi] = PB[2, hi] + OPP[1]
        if s == NS - 1:
            for h in both:
                dw_part(XTD, h, s, end_ref, h)
            arrive(now)
            arrive(late)
            dx_ref[...] = (PB[3] + FULL[0] + FULL[1]).astype(dx_ref.dtype)
        for h in both:
            if s < NS - 1:
                total(h, s).wait_recv()
                dw_add(h, s)
        if s == 1:
            start(late)

    for s in range(NS):
        for h in both:
            gather(h, s).wait_send()
            forward(h, s).wait_send()
            if s < NS - 1:
                total(h, s).wait_send()
    for copy in [w_swap, own_dy, x_swap] + x1 + x2a + x2b + x3i + x4i + x3ii + x4ii + x3iii + x4iii + opp + now + late:
        copy.wait_send()
    for h in both:
        total(h, NS - 1).wait()


def write(dx_ref, dw_ref, end_ref, dx_out, dw_out, last, sem):
    O = dw_ref.shape[1]
    SW = O // (2 * NS)
    copies = []

    def put(src, dst):
        copies.append(pltpu.make_async_copy(src, dst, sem.at[len(copies)]))
        copies[-1].start()

    tops = [(h + 1) * (O // 2) - SW for h in range(2)]
    for h in range(2):
        at = pl.ds(h * (O // 2), O // 2 - SW)
        put(dw_ref.at[:, at], dw_out.at[:, at])
    put(dx_ref, dx_out)
    for h in range(2):
        at = pl.ds(tops[h], SW)
        last[h] = dw_ref[:, at] + end_ref[h]
        put(last.at[h], dw_out.at[:, at])
    for copy in copies:
        copy.wait()


def solution(mesh):
    n, rows = mesh.shape["col"], mesh.shape["row"]
    assert n == 4 and mesh.shape["data"] == n and rows == 2
    act_spec = P(("pod", "data", "row"), "col")
    wgt_spec = P(("pod", "row"), "col")

    def local_step(x, w, dy):
        T, O = dy.shape
        F = x.shape[1]
        CT, FH = rows * T, F // rows
        QT, SW = CT // n, O // (2 * NS)
        bf16, f32 = jnp.bfloat16, jnp.float32
        dma = pltpu.SemaphoreType.DMA
        any_spec = pl.BlockSpec(memory_space=pl.ANY)
        vmem_spec = pl.BlockSpec(memory_space=pltpu.VMEM)
        dx, dw, end, _ = pl.pallas_call(
            functools.partial(kernel, n, rows),
            out_shape=[pltpu.VMEM((T, F), bf16), pltpu.VMEM((FH, O), f32), pltpu.VMEM((2, FH, SW), f32),
                       jax.ShapeDtypeStruct(w.shape, bf16)],
            in_specs=[any_spec] * 3,
            out_specs=[vmem_spec] * 3 + [any_spec],
            scratch_shapes=[
                pltpu.VMEM((2 * CT, O), bf16),
                pltpu.VMEM((CT, FH), bf16),
                pltpu.VMEM((n, QT, FH), bf16),
                pltpu.VMEM((7, n, QT, FH), bf16),
                pltpu.VMEM((2, FH, 2 * CT), bf16),
                pltpu.VMEM((2, FH, 2 * CT), bf16),
                pltpu.VMEM((2 * NS, FH, SW), f32),
                pltpu.VMEM((n, T, F), f32),
                pltpu.VMEM((2, T // 2, F), f32),
                pltpu.VMEM((2, T, F), f32),
                pltpu.VMEM((NW, F // NW, O), bf16),
                dma, dma((3,)), dma((2,)), dma((NW,)), dma((2,)),
                dma((2, NS)), dma((2, NS)), dma((2, NS)), dma((2, NS)),
                dma((n - 1,)), dma((n - 1,)), dma((4,)), dma((4,)), dma((18,)), dma((18,)),
                dma((6,)), dma((6,)), dma((2, NS)), dma((2, NS)), pltpu.SemaphoreType.REGULAR,
            ],
            compiler_params=pltpu.CompilerParams(
                collective_id=0, has_side_effects=True, vmem_limit_bytes=56 * 1000 * 1000),
            cost_estimate=pl.CostEstimate(flops=16 * T * F * O * n // 4, bytes_accessed=4 * T * O, transcendentals=0),
        )(x, w, dy)
        dx, dw, end = [pltpu.with_memory_space_constraint(v, pltpu.VMEM) for v in (dx, dw, end)]
        return pl.pallas_call(
            write,
            out_shape=[jax.ShapeDtypeStruct((T, F), bf16), jax.ShapeDtypeStruct((FH, O), f32)],
            in_specs=[vmem_spec] * 3,
            out_specs=[any_spec] * 2,
            scratch_shapes=[pltpu.VMEM((2, FH, SW), f32), dma((5,))],
            compiler_params=pltpu.CompilerParams(vmem_limit_bytes=2 * 1000 * 1000),
        )(dx, dw, end)

    return jax.shard_map(local_step, mesh=mesh, in_specs=(act_spec, wgt_spec, act_spec), out_specs=(act_spec, act_spec),
                         check_vma=False)
```

```python
import functools

import jax
import jax.numpy as jnp
from jax import lax
from jax.experimental import pallas as pl
from jax.experimental.pallas import tpu as pltpu
from jax.sharding import PartitionSpec as P

MESH = pl.DeviceIdType.MESH
NS = 4
NW = 3


def kernel(n, rows, x_ref, w_ref, dy_ref, dx_ref, dw_ref, end_ref, ws_ref,
           DY, X0, X1, XA, XTP, XTD, RP, PB, OPP, FULL, WT,
           lsem, x0s, wx, wt, os, gs, gr, fs, fr, x1s, x1r, x2s, x2r, x3s, x3r, ps, pr, rs, rr, x4s, there):
    T, O = dy_ref.shape
    F = x_ref.shape[1]
    CT, TH, FH = rows * T, T // 2, F // rows
    QT, QH = CT // n, CT // n // 2
    SW, FT = O // (2 * NS), F // NW
    d, c, r = lax.axis_index("data"), lax.axis_index("col"), lax.axis_index("row")

    def mod(v):
        return lax.rem(v + 2 * n, n)

    cp, cm, sib = mod(c + 1), mod(c - 1), 1 - r
    pair = [d + 1 - 2 * lax.rem(d, 2), n - 1 - d]
    far = mod(d + 2)

    def remote(src, dst, ssem, rsem, **where):
        return pltpu.make_async_remote_copy(src_ref=src, dst_ref=dst, send_sem=ssem, recv_sem=rsem,
                                            device_id=where, device_id_type=MESH)

    def start(copies):
        for copy in copies:
            copy.start()

    def arrive(copies):
        for copy in copies:
            copy.wait_recv()

    mine = pl.ds(pl.multiple_of(r * T, T), T)
    other = pl.ds(pl.multiple_of(CT + r * T, T), T)

    def cols(h, s):
        return pl.ds(h * (O // 2) + s * SW, SW)

    load_dy = pltpu.make_async_copy(dy_ref, DY.at[mine, :], lsem)

    def gather(h, s):
        return remote(dy_ref.at[:, cols(h, s)], DY.at[other, cols(h, s)], gs, gr.at[h, s], data=pair[h])

    def forward(h, s):
        return remote(DY.at[other, cols(h, s)], DY.at[other, cols(h, s)], fs, fr.at[h, s], row=sib)

    own_dy = remote(dy_ref, DY.at[mine, :], os.at[0], os.at[1], row=sib)
    w_swap = remote(w_ref, ws_ref, wx.at[0], wx.at[1], row=sib)

    def feats(row):
        return pl.ds(pl.multiple_of(row * FH, FH), FH)

    x_keep = pltpu.make_async_copy(x_ref.at[:, feats(r)], X0.at[mine, :], x0s.at[0])
    x_swap = remote(x_ref.at[:, feats(sib)], X0.at[mine, :], x0s.at[1], x0s.at[2], row=sib)

    def quarter(j):
        return pl.ds(pl.multiple_of(j * QT, QT), QT)

    x1 = [remote(X0.at[quarter(mod(c + k)), :], X1.at[c], x1s, x1r.at[k - 1], col=mod(c + k))
          for k in range(1, n)]
    x2a = [remote(X1.at[far], XA.at[2 + h, c], x2s, x2r.at[h], data=pair[h]) for h in range(2)]
    x2b = [remote(X1.at[pair[h]], XA.at[5 + h, c], x2s, x2r.at[2 + h], data=pair[h]) for h in range(2)]

    slots = iter(range(64))

    def spread(src, dst):
        k, m = next(slots), next(slots)
        return [remote(src, dst, x3s, x3r.at[k], col=cp), remote(src, dst, x3s, x3r.at[m], col=cm)]

    def hand_on(right, left):
        k, m = next(slots), next(slots)
        return [remote(right, right, x3s, x3r.at[k], col=cp), remote(left, left, x3s, x3r.at[m], col=cm)]

    x3i = spread(X1.at[pair[1]], XA.at[0, c]) + spread(X1.at[pair[0]], XA.at[1, c])
    x4i = hand_on(XA.at[0, cm], XA.at[1, cp])
    x3ii = spread(XA.at[pl.ds(2, 2), c], XA.at[pl.ds(2, 2), c])
    x4ii = hand_on(XA.at[2, cm], XA.at[3, cp])
    x3iii = spread(X1.at[d], XA.at[4, c]) + spread(XA.at[pl.ds(5, 2), c], XA.at[pl.ds(5, 2), c])
    right, left = XA.at[4, cm, pl.ds(0, QH)], XA.at[4, cp, pl.ds(QH, QH)]
    halves = [remote(right, right, x4s.at[0], x3r.at[16], col=cp), remote(left, left, x4s.at[1], x3r.at[17], col=cm)]
    x4iii = (hand_on(XA.at[5, cm], XA.at[6, cp])
             + halves)

    lo, hi = pl.ds(0, TH), pl.ds(TH, TH)
    opp = [remote(PB.at[0, lo], OPP.at[0], ps, pr.at[0], col=cm),
           remote(PB.at[0, hi], OPP.at[1], ps, pr.at[1], col=cp)]
    now = [remote(PB.at[1, hi], FULL.at[0, hi], ps, pr.at[2], col=cm),
           remote(PB.at[2, lo], FULL.at[1, lo], ps, pr.at[3], col=cp)]
    late = [remote(PB.at[1, lo], FULL.at[0, lo], ps, pr.at[4], col=cm),
            remote(PB.at[2, hi], FULL.at[1, hi], ps, pr.at[5], col=cp)]

    def total(h, s):
        return remote(RP.at[h * NS + s], dw_ref.at[:, cols(h, s)], rs, rr.at[h, s], data=pair[1 - h])

    target = [mod(c + 2), cm, cp, c]
    per = n // rows

    def tile_wait(i):
        pltpu.make_async_copy(w_ref.at[pl.ds(0, FT), :], WT.at[i], wt.at[i]).wait()

    def tile_start(k, i):
        b = target[k]
        row0 = pl.multiple_of(lax.rem(b, per) * F + i * FT, FT)

        @pl.when(b // per == r)
        def _():
            pltpu.make_async_copy(w_ref.at[pl.ds(row0, FT), :], WT.at[i], wt.at[i]).start()

        @pl.when(b // per != r)
        def _():
            pltpu.make_async_copy(ws_ref.at[pl.ds(row0, FT), :], WT.at[i], wt.at[i]).start()

    def dx_block(k):
        def one(i, carry):
            tile_wait(i)
            PB[k, :, pl.ds(pl.multiple_of(i * FT, FT), FT)] = lax.dot_general(
                DY[mine, :], WT[i], (((1,), (1,)), ((), ())), preferred_element_type=jnp.float32)
            if k + 1 < n:
                tile_start(k + 1, i)
            return carry

        lax.fori_loop(0, NW, one, 0)

    half = SW // 2

    def product(xt, h, s, i):
        return lax.dot_general(xt, DY[:, pl.ds(pl.multiple_of(h * (O // 2) + s * SW + i * half, half), half)],
                               (((1,), (0,)), ((), ())), preferred_element_type=jnp.float32)

    def dw_part(xt, h, s, out, slot):
        def one(i, carry):
            out[slot, :, pl.ds(pl.multiple_of(i * half, half), half)] = product(xt[h], h, s, i)
            return carry

        lax.fori_loop(0, 2, one, 0)

    def dw_add(h, s):
        def one(i, carry):
            at = pl.ds(pl.multiple_of(h * (O // 2) + s * SW + i * half, half), half)
            dw_ref[:, at] = dw_ref[:, at] + product(XTD[h], h, s, i)
            return carry

        lax.fori_loop(0, 2, one, 0)

    def turn(block, places):
        for j in range(n):
            value = XA[block, j].T
            for ref, h, side in places:
                ref[h, :, pl.ds(side * CT + j * QT, QT)] = value

    both = range(2)
    barrier = pltpu.get_barrier_semaphore()
    early = r == 1

    def greet(**where):
        pl.semaphore_signal(barrier, inc=1, device_id=where, device_id_type=MESH)

    for p in pair:
        greet(data=p)


    @pl.when(early)
    def _():
        pl.semaphore_wait(barrier, 2)
        for h in both:
            gather(h, 0).start()
        greet(row=sib)
        for k in range(1, n):
            greet(col=mod(c + k), row=sib)

    @pl.when(jnp.logical_not(early))
    def _():
        for k in range(1, n):
            greet(col=mod(c + k))
        pl.semaphore_wait(barrier, 2 + 1 + 2 * (n - 1))
        pl.semaphore_signal(there, inc=1, device_id={"row": sib}, device_id_type=MESH)


    @pl.when(jnp.logical_not(early))
    def _():
        for h in both:
            gather(h, 0).start()

    for h in both:
        gather(h, 1).start()
    load_dy.start()
    x_keep.start()

    @pl.when(early)
    def _():
        pl.semaphore_wait(there, 1)

    x_swap.start()
    w_swap.start()
    x_keep.wait()
    x_swap.wait_recv()

    start(x1)
    X1[c] = X0[quarter(c), :]
    own_dy.start()
    arrive(x1)
    start(x3i)
    start(x2a)
    start(x2b)
    for s in range(2, NS):
        for h in both:
            gather(h, s).start()
    XA[0, c] = X1[pair[1]]
    XA[1, c] = X1[pair[0]]
    XA[4, c] = X1[d]
    for h in both:
        gather(h, 0).wait_recv()
        forward(h, 0).start()
    arrive(x2a)
    start(x3ii)
    arrive(x3i)
    start(x4i)
    load_dy.wait()
    w_swap.wait_recv()
    for i in range(NW):
        tile_start(0, i)
    dx_block(0)
    for h in both:
        gather(h, 1).wait_recv()
        forward(h, 1).start()
    arrive(x3ii)
    start(x4ii)
    dx_block(1)
    arrive(x2b)
    start(x3iii)
    dx_block(2)
    arrive(x4i)
    turn(0, [(XTP, 0, 0)])
    turn(1, [(XTP, 1, 0)])
    arrive(x4ii)
    turn(2, [(XTP, 0, 1)])
    turn(3, [(XTP, 1, 1)])
    own_dy.wait_recv()
    for s in range(NS):
        if s + 2 < NS:
            for h in both:
                gather(h, s + 2).wait_recv()
                forward(h, s + 2).start()
        for h in both:
            forward(h, s).wait_recv()
            dw_part(XTP, h, s, RP, h * NS + s)
        if s == 1:
            arrive(x3iii)
            start(x4iii)
            start(opp)
            start(now)
        for h in both:
            total(h, s).start()
    dx_block(3)
    arrive(x4iii)
    turn(4, [(XTD, 0, 0), (XTD, 1, 0)])
    turn(5, [(XTD, 0, 1)])
    turn(6, [(XTD, 1, 1)])
    for s in range(NS):
        if s == 1:
            arrive(opp)
            PB[1, lo] = PB[1, lo] + OPP[0]
            PB[2, hi] = PB[2, hi] + OPP[1]
        if s == NS - 1:
            for h in both:
                dw_part(XTD, h, s, end_ref, h)
            arrive(now)
            arrive(late)
            dx_ref[...] = (PB[3] + FULL[0] + FULL[1]).astype(dx_ref.dtype)
        for h in both:
            if s < NS - 1:
                total(h, s).wait_recv()
                dw_add(h, s)
        if s == 1:
            start(late)

    for sem, ref in ((gs, dy_ref), (fs, DY.at[other, :]), (rs, RP), (ps, PB.at[pl.ds(0, 3)]),
                      (x1s, X1.at[pl.ds(0, n - 1)]), (x2s, X1), (x3s, XA.at[pl.ds(0, 5)])):
        pltpu.make_async_copy(ref, ref, sem).wait()
    for copy in [w_swap, own_dy, x_swap] + halves:
        copy.wait_send()
    for h in both:
        total(h, NS - 1).wait_recv()


def write(dx_ref, dw_ref, end_ref, dx_out, dw_out, last, sem):
    O = dw_ref.shape[1]
    SW = O // (2 * NS)
    copies = []

    def put(src, dst):
        copies.append(pltpu.make_async_copy(src, dst, sem.at[len(copies)]))
        copies[-1].start()

    tops = [(h + 1) * (O // 2) - SW for h in range(2)]
    for h in range(2):
        at = pl.ds(h * (O // 2), O // 2 - SW)
        put(dw_ref.at[:, at], dw_out.at[:, at])
    put(dx_ref, dx_out)
    for h in range(2):
        at = pl.ds(tops[h], SW)
        last[h] = dw_ref[:, at] + end_ref[h]
        put(last.at[h], dw_out.at[:, at])
    for copy in copies:
        copy.wait()


def solution(mesh):
    n, rows = mesh.shape["col"], mesh.shape["row"]
    assert n == 4 and mesh.shape["data"] == n and rows == 2
    act_spec = P(("pod", "data", "row"), "col")
    wgt_spec = P(("pod", "row"), "col")

    def local_step(x, w, dy):
        T, O = dy.shape
        F = x.shape[1]
        CT, FH = rows * T, F // rows
        QT, SW = CT // n, O // (2 * NS)
        bf16, f32 = jnp.bfloat16, jnp.float32
        dma = pltpu.SemaphoreType.DMA
        any_spec = pl.BlockSpec(memory_space=pl.ANY)
        vmem_spec = pl.BlockSpec(memory_space=pltpu.VMEM)
        dx, dw, end, _ = pl.pallas_call(
            functools.partial(kernel, n, rows),
            out_shape=[pltpu.VMEM((T, F), bf16), pltpu.VMEM((FH, O), f32), pltpu.VMEM((2, FH, SW), f32),
                       jax.ShapeDtypeStruct(w.shape, bf16)],
            in_specs=[any_spec] * 3,
            out_specs=[vmem_spec] * 3 + [any_spec],
            scratch_shapes=[
                pltpu.VMEM((2 * CT, O), bf16),
                pltpu.VMEM((CT, FH), bf16),
                pltpu.VMEM((n, QT, FH), bf16),
                pltpu.VMEM((7, n, QT, FH), bf16),
                pltpu.VMEM((2, FH, 2 * CT), bf16),
                pltpu.VMEM((2, FH, 2 * CT), bf16),
                pltpu.VMEM((2 * NS, FH, SW), f32),
                pltpu.VMEM((n, T, F), f32),
                pltpu.VMEM((2, T // 2, F), f32),
                pltpu.VMEM((2, T, F), f32),
                pltpu.VMEM((NW, F // NW, O), bf16),
                dma, dma((3,)), dma((2,)), dma((NW,)), dma((2,)),
                dma, dma((2, NS)), dma, dma((2, NS)),
                dma, dma((n - 1,)), dma, dma((4,)), dma, dma((18,)),
                dma, dma((6,)), dma, dma((2, NS)), dma((2,)), pltpu.SemaphoreType.REGULAR,
            ],
            compiler_params=pltpu.CompilerParams(
                collective_id=0, has_side_effects=True, vmem_limit_bytes=56 * 1000 * 1000),
            cost_estimate=pl.CostEstimate(flops=16 * T * F * O * n // 4, bytes_accessed=4 * T * O, transcendentals=0),
        )(x, w, dy)
        dx, dw, end = [pltpu.with_memory_space_constraint(v, pltpu.VMEM) for v in (dx, dw, end)]
        return pl.pallas_call(
            write,
            out_shape=[jax.ShapeDtypeStruct((T, F), bf16), jax.ShapeDtypeStruct((FH, O), f32)],
            in_specs=[vmem_spec] * 3,
            out_specs=[any_spec] * 2,
            scratch_shapes=[pltpu.VMEM((2, FH, SW), f32), dma((5,))],
            compiler_params=pltpu.CompilerParams(vmem_limit_bytes=2 * 1000 * 1000),
        )(dx, dw, end)

    return jax.shard_map(local_step, mesh=mesh, in_specs=(act_spec, wgt_spec, act_spec), out_specs=(act_spec, act_spec),
                         check_vma=False)
```

```python
import functools

import jax
import jax.numpy as jnp
from jax import lax
from jax.experimental import pallas as pl
from jax.experimental.pallas import tpu as pltpu
from jax.sharding import PartitionSpec as P

MESH = pl.DeviceIdType.MESH
NS = 4
NW = 3


def kernel(n, rows, x_ref, w_ref, dy_ref, dx_ref, dw_ref, end_ref, ws_ref,
           DY, X0, X1, XA, XTP, XTD, RP, PB, OPP, FULL, WT,
           lsem, x0s, wx, wt, os, gs, gr, fs, fr, x1s, x1r, x2s, x2r, x3s, x3r, ps, pr, rs, rr, x4s, there):
    T, O = dy_ref.shape
    F = x_ref.shape[1]
    CT, TH, FH = rows * T, T // 2, F // rows
    QT, QH = CT // n, CT // n // 2
    SW, FT = O // (2 * NS), F // NW
    d, c, r = lax.axis_index("data"), lax.axis_index("col"), lax.axis_index("row")

    def mod(v):
        return lax.rem(v + 2 * n, n)

    cp, cm, sib = mod(c + 1), mod(c - 1), 1 - r
    pair = [d + 1 - 2 * lax.rem(d, 2), n - 1 - d]
    far = mod(d + 2)

    def remote(src, dst, ssem, rsem, **where):
        return pltpu.make_async_remote_copy(src_ref=src, dst_ref=dst, send_sem=ssem, recv_sem=rsem,
                                            device_id=where, device_id_type=MESH)

    def start(copies):
        for copy in copies:
            copy.start()

    def arrive_all(ref, sem):
        pltpu.make_async_copy(ref, ref, sem).wait()

    def arrive(copies):
        for copy in copies:
            copy.wait_recv()

    mine = pl.ds(pl.multiple_of(r * T, T), T)
    other = pl.ds(pl.multiple_of(CT + r * T, T), T)

    def cols(h, s):
        return pl.ds(h * (O // 2) + s * SW, SW)

    load_dy = pltpu.make_async_copy(dy_ref, DY.at[mine, :], lsem)

    def gather(h, s):
        return remote(dy_ref.at[:, cols(h, s)], DY.at[other, cols(h, s)], gs, gr.at[h, s], data=pair[h])

    def forward(h, s):
        return remote(DY.at[other, cols(h, s)], DY.at[other, cols(h, s)], fs, fr.at[h, s], row=sib)

    own_dy = remote(dy_ref, DY.at[mine, :], os.at[0], os.at[1], row=sib)
    w_swap = remote(w_ref, ws_ref, wx.at[0], wx.at[1], row=sib)

    def feats(row):
        return pl.ds(pl.multiple_of(row * FH, FH), FH)

    x_keep = pltpu.make_async_copy(x_ref.at[:, feats(r)], X0.at[mine, :], x0s.at[0])
    x_swap = remote(x_ref.at[:, feats(sib)], X0.at[mine, :], x0s.at[1], x0s.at[2], row=sib)

    def quarter(j):
        return pl.ds(pl.multiple_of(j * QT, QT), QT)

    x1 = [remote(X0.at[quarter(mod(c + k)), :], X1.at[c], x1s, x1r, col=mod(c + k))
          for k in range(1, n)]
    x2a = [remote(X1.at[far], XA.at[2 + h, c], x2s, x2r.at[0], data=pair[h]) for h in range(2)]
    x2b = [remote(X1.at[pair[h]], XA.at[5 + h, c], x2s, x2r.at[1], data=pair[h]) for h in range(2)]

    slots = iter(range(64))

    def spread(src, dst):
        k, m = next(slots), next(slots)
        return [remote(src, dst, x3s, x3r.at[k], col=cp), remote(src, dst, x3s, x3r.at[m], col=cm)]

    def hand_on(right, left):
        k, m = next(slots), next(slots)
        return [remote(right, right, x3s, x3r.at[k], col=cp), remote(left, left, x3s, x3r.at[m], col=cm)]

    x3i = spread(X1.at[pair[1]], XA.at[0, c]) + spread(X1.at[pair[0]], XA.at[1, c])
    x4i = hand_on(XA.at[0, cm], XA.at[1, cp])
    x3ii = spread(XA.at[pl.ds(2, 2), c], XA.at[pl.ds(2, 2), c])
    x4ii = hand_on(XA.at[2, cm], XA.at[3, cp])
    x3iii = spread(X1.at[d], XA.at[4, c]) + spread(XA.at[pl.ds(5, 2), c], XA.at[pl.ds(5, 2), c])
    right, left = XA.at[4, cm, pl.ds(0, QH)], XA.at[4, cp, pl.ds(QH, QH)]
    halves = [remote(right, right, x4s.at[0], x3r.at[16], col=cp), remote(left, left, x4s.at[1], x3r.at[17], col=cm)]
    x4iii = (hand_on(XA.at[5, cm], XA.at[6, cp])
             + halves)

    lo, hi = pl.ds(0, TH), pl.ds(TH, TH)
    opp = [remote(PB.at[0, lo], OPP.at[0], ps, pr.at[0], col=cm),
           remote(PB.at[0, hi], OPP.at[1], ps, pr.at[0], col=cp)]
    now = [remote(PB.at[1, hi], FULL.at[0, hi], ps, pr.at[1], col=cm),
           remote(PB.at[2, lo], FULL.at[1, lo], ps, pr.at[1], col=cp)]
    late = [remote(PB.at[1, lo], FULL.at[0, lo], ps, pr.at[1], col=cm),
            remote(PB.at[2, hi], FULL.at[1, hi], ps, pr.at[1], col=cp)]

    def total(h, s):
        return remote(RP.at[h * NS + s], dw_ref.at[:, cols(h, s)], rs, rr.at[h, s], data=pair[1 - h])

    target = [mod(c + 2), cm, cp, c]
    per = n // rows

    def tile_wait(i):
        pltpu.make_async_copy(w_ref.at[pl.ds(0, FT), :], WT.at[i], wt.at[i]).wait()

    def tile_start(k, i):
        b = target[k]
        row0 = pl.multiple_of(lax.rem(b, per) * F + i * FT, FT)

        @pl.when(b // per == r)
        def _():
            pltpu.make_async_copy(w_ref.at[pl.ds(row0, FT), :], WT.at[i], wt.at[i]).start()

        @pl.when(b // per != r)
        def _():
            pltpu.make_async_copy(ws_ref.at[pl.ds(row0, FT), :], WT.at[i], wt.at[i]).start()

    def dx_block(k):
        def one(i, carry):
            tile_wait(i)
            PB[k, :, pl.ds(pl.multiple_of(i * FT, FT), FT)] = lax.dot_general(
                DY[mine, :], WT[i], (((1,), (1,)), ((), ())), preferred_element_type=jnp.float32)
            if k + 1 < n:
                tile_start(k + 1, i)
            return carry

        lax.fori_loop(0, NW, one, 0)

    half = SW // 2

    def product(xt, h, s, i):
        return lax.dot_general(xt, DY[:, pl.ds(pl.multiple_of(h * (O // 2) + s * SW + i * half, half), half)],
                               (((1,), (0,)), ((), ())), preferred_element_type=jnp.float32)

    def dw_part(xt, h, s, out, slot):
        def one(i, carry):
            out[slot, :, pl.ds(pl.multiple_of(i * half, half), half)] = product(xt[h], h, s, i)
            return carry

        lax.fori_loop(0, 2, one, 0)

    def dw_add(h, s):
        def one(i, carry):
            at = pl.ds(pl.multiple_of(h * (O // 2) + s * SW + i * half, half), half)
            dw_ref[:, at] = dw_ref[:, at] + product(XTD[h], h, s, i)
            return carry

        lax.fori_loop(0, 2, one, 0)

    def turn(block, places):
        for j in range(n):
            value = XA[block, j].T
            for ref, h, side in places:
                ref[h, :, pl.ds(side * CT + j * QT, QT)] = value

    both = range(2)
    barrier = pltpu.get_barrier_semaphore()
    early = r == 1

    def greet(**where):
        pl.semaphore_signal(barrier, inc=1, device_id=where, device_id_type=MESH)

    for p in pair:
        greet(data=p)


    @pl.when(early)
    def _():
        pl.semaphore_wait(barrier, 2)
        for h in both:
            gather(h, 0).start()
        greet(row=sib)
        for k in range(1, n):
            greet(col=mod(c + k), row=sib)

    @pl.when(jnp.logical_not(early))
    def _():
        for k in range(1, n):
            greet(col=mod(c + k))
        pl.semaphore_wait(barrier, 2 + 1 + 2 * (n - 1))
        pl.semaphore_signal(there, inc=1, device_id={"row": sib}, device_id_type=MESH)


    @pl.when(jnp.logical_not(early))
    def _():
        for h in both:
            gather(h, 0).start()

    for h in both:
        gather(h, 1).start()
    load_dy.start()
    x_keep.start()

    @pl.when(early)
    def _():
        pl.semaphore_wait(there, 1)

    x_swap.start()
    w_swap.start()
    x_keep.wait()
    x_swap.wait_recv()

    start(x1)
    X1[c] = X0[quarter(c), :]
    own_dy.start()
    arrive_all(X1.at[pl.ds(0, n - 1)], x1r)
    start(x3i)
    start(x2a)
    start(x2b)
    for s in range(2, NS):
        for h in both:
            gather(h, s).start()
    XA[0, c] = X1[pair[1]]
    XA[1, c] = X1[pair[0]]
    XA[4, c] = X1[d]
    for h in both:
        gather(h, 0).wait_recv()
        forward(h, 0).start()
    arrive_all(X1.at[pl.ds(0, 2)], x2r.at[0])
    start(x3ii)
    arrive(x3i)
    start(x4i)
    load_dy.wait()
    w_swap.wait_recv()
    for i in range(NW):
        tile_start(0, i)
    dx_block(0)
    for h in both:
        gather(h, 1).wait_recv()
        forward(h, 1).start()
    arrive(x3ii)
    start(x4ii)
    dx_block(1)
    arrive_all(X1.at[pl.ds(0, 2)], x2r.at[1])
    start(x3iii)
    dx_block(2)
    arrive(x4i)
    turn(0, [(XTP, 0, 0)])
    turn(1, [(XTP, 1, 0)])
    arrive(x4ii)
    turn(2, [(XTP, 0, 1)])
    turn(3, [(XTP, 1, 1)])
    own_dy.wait_recv()
    for s in range(NS):
        if s + 2 < NS:
            for h in both:
                gather(h, s + 2).wait_recv()
                forward(h, s + 2).start()
        for h in both:
            forward(h, s).wait_recv()
            dw_part(XTP, h, s, RP, h * NS + s)
        if s == 1:
            arrive(x3iii)
            start(x4iii)
            start(opp)
            start(now)
        for h in both:
            total(h, s).start()
    dx_block(3)
    arrive(x4iii)
    turn(4, [(XTD, 0, 0), (XTD, 1, 0)])
    turn(5, [(XTD, 0, 1)])
    turn(6, [(XTD, 1, 1)])
    for s in range(NS):
        if s == 1:
            arrive_all(OPP, pr.at[0])
            PB[1, lo] = PB[1, lo] + OPP[0]
            PB[2, hi] = PB[2, hi] + OPP[1]
        if s == NS - 1:
            for h in both:
                dw_part(XTD, h, s, end_ref, h)
            arrive_all(FULL, pr.at[1])
            dx_ref[...] = (PB[3] + FULL[0] + FULL[1]).astype(dx_ref.dtype)
        for h in both:
            if s < NS - 1:
                total(h, s).wait_recv()
                dw_add(h, s)
        if s == 1:
            start(late)

    for sem, ref in ((gs, dy_ref), (fs, DY.at[other, :]), (rs, RP), (ps, PB.at[pl.ds(0, 3)]),
                      (x1s, X1.at[pl.ds(0, n - 1)]), (x2s, X1), (x3s, XA.at[pl.ds(0, 5)])):
        pltpu.make_async_copy(ref, ref, sem).wait()
    for copy in [w_swap, own_dy, x_swap] + halves:
        copy.wait_send()
    for h in both:
        total(h, NS - 1).wait_recv()


def write(dx_ref, dw_ref, end_ref, dx_out, dw_out, last, sem):
    O = dw_ref.shape[1]
    SW = O // (2 * NS)
    copies = []

    def put(src, dst):
        copies.append(pltpu.make_async_copy(src, dst, sem.at[len(copies)]))
        copies[-1].start()

    tops = [(h + 1) * (O // 2) - SW for h in range(2)]
    for h in range(2):
        at = pl.ds(h * (O // 2), O // 2 - SW)
        put(dw_ref.at[:, at], dw_out.at[:, at])
    put(dx_ref, dx_out)
    for h in range(2):
        at = pl.ds(tops[h], SW)
        last[h] = dw_ref[:, at] + end_ref[h]
        put(last.at[h], dw_out.at[:, at])
    for copy in copies:
        copy.wait()


def solution(mesh):
    n, rows = mesh.shape["col"], mesh.shape["row"]
    assert n == 4 and mesh.shape["data"] == n and rows == 2
    act_spec = P(("pod", "data", "row"), "col")
    wgt_spec = P(("pod", "row"), "col")

    def local_step(x, w, dy):
        T, O = dy.shape
        F = x.shape[1]
        CT, FH = rows * T, F // rows
        QT, SW = CT // n, O // (2 * NS)
        bf16, f32 = jnp.bfloat16, jnp.float32
        dma = pltpu.SemaphoreType.DMA
        any_spec = pl.BlockSpec(memory_space=pl.ANY)
        vmem_spec = pl.BlockSpec(memory_space=pltpu.VMEM)
        dx, dw, end, _ = pl.pallas_call(
            functools.partial(kernel, n, rows),
            out_shape=[pltpu.VMEM((T, F), bf16), pltpu.VMEM((FH, O), f32), pltpu.VMEM((2, FH, SW), f32),
                       jax.ShapeDtypeStruct(w.shape, bf16)],
            in_specs=[any_spec] * 3,
            out_specs=[vmem_spec] * 3 + [any_spec],
            scratch_shapes=[
                pltpu.VMEM((2 * CT, O), bf16),
                pltpu.VMEM((CT, FH), bf16),
                pltpu.VMEM((n, QT, FH), bf16),
                pltpu.VMEM((7, n, QT, FH), bf16),
                pltpu.VMEM((2, FH, 2 * CT), bf16),
                pltpu.VMEM((2, FH, 2 * CT), bf16),
                pltpu.VMEM((2 * NS, FH, SW), f32),
                pltpu.VMEM((n, T, F), f32),
                pltpu.VMEM((2, T // 2, F), f32),
                pltpu.VMEM((2, T, F), f32),
                pltpu.VMEM((NW, F // NW, O), bf16),
                dma, dma((3,)), dma((2,)), dma((NW,)), dma((2,)),
                dma, dma((2, NS)), dma, dma((2, NS)),
                dma, dma, dma, dma((2,)), dma, dma((18,)),
                dma, dma((2,)), dma, dma((2, NS)), dma((2,)), pltpu.SemaphoreType.REGULAR,
            ],
            compiler_params=pltpu.CompilerParams(
                collective_id=0, has_side_effects=True, vmem_limit_bytes=56 * 1000 * 1000),
            cost_estimate=pl.CostEstimate(flops=16 * T * F * O * n // 4, bytes_accessed=4 * T * O, transcendentals=0),
        )(x, w, dy)
        dx, dw, end = [pltpu.with_memory_space_constraint(v, pltpu.VMEM) for v in (dx, dw, end)]
        return pl.pallas_call(
            write,
            out_shape=[jax.ShapeDtypeStruct((T, F), bf16), jax.ShapeDtypeStruct((FH, O), f32)],
            in_specs=[vmem_spec] * 3,
            out_specs=[any_spec] * 2,
            scratch_shapes=[pltpu.VMEM((2, FH, SW), f32), dma((5,))],
            compiler_params=pltpu.CompilerParams(vmem_limit_bytes=2 * 1000 * 1000),
        )(dx, dw, end)

    return jax.shard_map(local_step, mesh=mesh, in_specs=(act_spec, wgt_spec, act_spec), out_specs=(act_spec, act_spec),
                         check_vma=False)
```
